128 devices in a mesh: section: 2 (over x_hi), grp: 64 (over y, z, x_lo, core).
Axes of the slice: x: 4 (x_hi: 2, x_lo: 2; x = x_hi * 2 + x_lo), y: 4, z: 4, core: 2. Of those that a mesh axis runs over, the one named last changes fastest.
Arguments:
- voltages: bfloat16 [1024, 524288], P('grp', 'section'), may hold values from -6 to 6
- filter_taps: float32 [8, 512], replicated, may hold values from -2 to 2
- beam_weights: bfloat16 [256, 2, 512, 1024], P('grp'), may hold values from -0.125 to 0.125
- antenna_of_row: int32 [1024], replicated, may hold values from 0 to 1023, each once
- beam_delay: int32 [512], P('grp'), may hold values from 0 to 127
Outputs:
- dedispersed: float32 [256, 2, 512, 1024], P(None, None, 'grp', 'section')
The draws below stay inside these ranges and needn't reach their ends.
Inputs may be any that keep to these rules, and one draw needn't show every extreme that they name: A permutation: voltage row r holds physical antenna antenna_of_row[r].
All inputs are finite; a program needn't handle non-finite values.
Results may differ from the reference program's by a relative error of at most 0.0069.
Values may be sent and summed in bfloat16 or wider, within the bound.
A program may use at most 128 MiB of HBM per device.

```python
import math
import jax
import jax.numpy as jnp
from jax import lax

ANTENNAS = 1024
FRAME = 512
CHANNELS = 256
TAPS = 8
BEAMS = 512
DFT_LEN = 256
ADVANCE = 128
SPECTRA = 1024
SAMPLES = 524288


def plant(values, rng, low, high):
    dims = values.shape
    spot = [jax.random.randint(jax.random.fold_in(rng, axis), (), 0, dims[axis]) for axis in range(len(dims))]
    values = values.at[tuple(spot)].set(low)
    longest = dims.index(max(dims))
    spot[longest] = (spot[longest] + 1) % dims[longest]
    return values.at[tuple(spot)].set(high)


def shard_levels(own_key, dims, split, least, largest):
    level = 1.0
    for position, parts in split:
        steps = jax.random.uniform(jax.random.fold_in(jax.random.fold_in(own_key, 6), position), (parts,), jnp.float32, least / len(split), largest / len(split))
        level = level * jnp.repeat(jnp.exp(steps), dims[position] // parts).reshape((-1,) + (1,) * (len(dims) - 1 - position))
    return level


def gaussian(stream_key, extent, spread, bound, pieces=(), kind=jnp.bfloat16):
    values = jax.random.normal(stream_key, extent, jnp.float32) * spread
    if len(pieces) > 0:
        values = shard_levels(stream_key, extent, pieces, -0.22, 0.18) * values
    return jnp.clip(values, min=-bound, max=bound).astype(kind)


def setup_inputs(seed: int = 0) -> dict:
    key_of = jax.random.split(jax.random.key(seed), 6)
    voltages = gaussian(key_of[0], (ANTENNAS, SAMPLES), 1.0, 6.0, ((0, 64), (1, 2)))
    filter_taps = gaussian(key_of[1], (TAPS, FRAME), TAPS ** -0.5, 2.0, (), jnp.float32)
    beam_weights = gaussian(key_of[2], (CHANNELS, 2, BEAMS, ANTENNAS), (2 * ANTENNAS) ** -0.5, 0.125, ((0, 64),))
    antenna_of_row = jax.random.permutation(key_of[3], ANTENNAS).astype(jnp.int32)
    beam_delay = plant(jax.random.randint(key_of[4], (BEAMS,), 0, DFT_LEN // 2), jax.random.fold_in(key_of[4], 1), 0, (DFT_LEN // 2) - 1).astype(jnp.int32)
    return dict(voltages=voltages, filter_taps=filter_taps, beam_weights=beam_weights, antenna_of_row=antenna_of_row, beam_delay=beam_delay)


def rounded(values):
    return lax.optimization_barrier(values.astype(jnp.bfloat16))


def channel_table(frame_length):
    channels = frame_length // 2
    column = jnp.arange(frame_length, dtype=jnp.int32)
    channel = column % channels
    quadrature = column // channels
    sample = jnp.arange(frame_length, dtype=jnp.int32)[:, None]
    winding = (sample * channel[None, :]) % frame_length
    angles = (2.0 * math.pi / frame_length) * winding.astype(jnp.float32)
    factor = channels ** -0.5
    dft_cols = jnp.where(quadrature[None, :] == 0, jnp.cos(angles) * factor, -jnp.sin(angles) * factor)
    return dft_cols.astype(jnp.bfloat16)


def block_tables(length):
    half_len = length // 2
    factor = length ** -0.5
    sample = jnp.arange(length, dtype=jnp.int32)
    angles = (2.0 * math.pi / length) * ((sample[:, None] * sample[None, :]) % length).astype(jnp.float32)
    cosine_table = (jnp.cos(angles) * factor).astype(jnp.bfloat16)
    sine_table = (jnp.sin(angles) * factor).astype(jnp.bfloat16)
    forward_real = jnp.concatenate([cosine_table, -sine_table], axis=1)
    forward_imag = jnp.concatenate([sine_table, cosine_table], axis=1)
    back_cos = cosine_table[:, half_len:]
    back_sin = sine_table[:, half_len:]
    inverse_real = jnp.concatenate([back_cos, back_sin], axis=1)
    inverse_imag = jnp.concatenate([-back_sin, back_cos], axis=1)
    return forward_real, forward_imag, inverse_real, inverse_imag


def chirp_factor(delays, channel_start, channel_count, channels, length):
    frequency = jnp.arange(length, dtype=jnp.int32)
    signed = jnp.where(frequency < length // 2, frequency, frequency - length).astype(jnp.float32)
    channel = (channel_start + jnp.arange(channel_count, dtype=jnp.int32)).astype(jnp.float32)
    strength = (1.0 + channel / channels) ** -3.0
    sweep = signed * signed / (length * length)
    phases = (math.pi * delays.astype(jnp.float32))[None, :, None] * strength[:, None, None] * sweep[None, None, :] - (0.5 * math.pi) * frequency.astype(jnp.float32)[None, None, :]
    return jnp.cos(phases), jnp.sin(phases)


def channelise(antenna_block, filter_taps, dft_cols):
    row_count = antenna_block.shape[0]
    past_samples = jnp.zeros((row_count, (TAPS - 1) * FRAME), jnp.bfloat16)
    extended = jnp.concatenate([past_samples, antenna_block], axis=1).reshape(row_count, SPECTRA + TAPS - 1, FRAME)
    weighted = jnp.zeros((row_count, SPECTRA, FRAME), jnp.float32)
    for tap_index in range(TAPS):
        weighted = weighted + filter_taps[tap_index] * extended[:, tap_index:tap_index + SPECTRA, :].astype(jnp.float32)
    weighted = rounded(weighted)
    product = jnp.einsum("asp,pj->ajs", weighted.astype(jnp.float32), dft_cols.astype(jnp.float32), precision=lax.Precision.HIGHEST)
    return rounded(product)


def reference(voltages, filter_taps, beam_weights, antenna_of_row, beam_delay):
    dft_cols = channel_table(FRAME)
    block_rows = math.gcd(ANTENNAS, 64)
    grouped = voltages.reshape(ANTENNAS // block_rows, block_rows, SAMPLES)
    channelised = lax.map(lambda antenna_block: channelise(antenna_block, filter_taps, dft_cols), grouped)
    channelised = channelised.reshape(ANTENNAS, FRAME, SPECTRA)
    by_column = jnp.moveaxis(channelised, 1, 0)

    def form_channel(inputs):
        steering_weights, part_real, part_imag = inputs
        ordered = jnp.take(steering_weights, antenna_of_row, axis=2).astype(jnp.float32)
        real_in = part_real.astype(jnp.float32)
        imag_in = part_imag.astype(jnp.float32)
        beam_real = jnp.dot(ordered[0], real_in, precision=lax.Precision.HIGHEST) - jnp.dot(ordered[1], imag_in, precision=lax.Precision.HIGHEST)
        beam_imag = jnp.dot(ordered[0], imag_in, precision=lax.Precision.HIGHEST) + jnp.dot(ordered[1], real_in, precision=lax.Precision.HIGHEST)
        return rounded(jnp.stack([beam_real, beam_imag]))

    beamed = lax.map(form_channel, (beam_weights, by_column[:CHANNELS], by_column[CHANNELS:]))
    forward_real, forward_imag, inverse_real, inverse_imag = [table_part.astype(jnp.float32) for table_part in block_tables(DFT_LEN)]

    def dedisperse_channel(inputs):
        series, channel = inputs
        block_count = SPECTRA // ADVANCE
        leading = jnp.zeros((2, BEAMS, ADVANCE), jnp.bfloat16)
        joined = jnp.concatenate([leading, series], axis=2).reshape(2, BEAMS, block_count + 1, ADVANCE)
        blocks = jnp.concatenate([joined[:, :, :-1, :], joined[:, :, 1:, :]], axis=3).astype(jnp.float32)
        spectrum = jnp.einsum("bml,lk->bmk", blocks[0], forward_real, precision=lax.Precision.HIGHEST) + jnp.einsum("bml,lk->bmk", blocks[1], forward_imag, precision=lax.Precision.HIGHEST)
        chirp_real, chirp_imag = chirp_factor(beam_delay, channel, 1, CHANNELS, DFT_LEN)
        chirp_real = chirp_real[0][:, None, :]
        chirp_imag = chirp_imag[0][:, None, :]
        spec_real = spectrum[:, :, :DFT_LEN]
        spec_imag = spectrum[:, :, DFT_LEN:]
        filtered_real = rounded(spec_real * chirp_real - spec_imag * chirp_imag).astype(jnp.float32)
        filtered_imag = rounded(spec_real * chirp_imag + spec_imag * chirp_real).astype(jnp.float32)
        result = jnp.einsum("bmk,kn->bmn", filtered_real, inverse_real, precision=lax.Precision.HIGHEST) + jnp.einsum("bmk,kn->bmn", filtered_imag, inverse_imag, precision=lax.Precision.HIGHEST)
        out_real = result[:, :, :ADVANCE].reshape(BEAMS, SPECTRA)
        out_imag = result[:, :, ADVANCE:].reshape(BEAMS, SPECTRA)
        return jnp.stack([out_real, out_imag])

    return lax.map(dedisperse_channel, (beamed, jnp.arange(CHANNELS, dtype=jnp.int32)))
```

```python
import functools
import math
import random

import jax
import jax.numpy as jnp
import numpy as np
from jax import lax
from jax.experimental import pallas as pl
from jax.experimental.pallas import tpu as pltpu
from jax.sharding import PartitionSpec as P

MESH = pl.DeviceIdType.MESH
F32 = jnp.float32
BF16 = jnp.bfloat16
NG = 64
NY, NZ, NX, NC = 4, 4, 2, 2
ANT = 16
FRAME = 512
HALF = FRAME // 2
TAPS = 8
CH = 256
CPD = CH // NG
CHUNKS = 4
SC = 128
LEAD = (TAPS - 1) * FRAME
BEAMS = 512
BPD = BEAMS // NG
ROWS = CH * BPD
ALL_ANT = ANT * NG
RT = 256


def send_order(seed=0):
    rng = random.Random(seed)
    left = [
        (dy, dz, dx, dc) for dy in range(NY) for dz in range(NZ) for dx in range(NX) for dc in range(NC)
    ][1:]
    rng.shuffle(left)
    load = {}

    def ports(o):
        p = []
        for name, d in (("y", o[0]), ("z", o[1])):
            if d in (1, 2):
                p.append(name + "+")
            if d in (2, 3):
                p.append(name + "-")
        if o[2]:
            p.append("x")
        return p

    out = []
    while left:
        best = min(
            left,
            key=lambda o: (max([load.get(p, 0) + 1 for p in ports(o)] + [0]), -len(ports(o)), rng.random()),
        )
        for p in ports(best):
            load[p] = load.get(p, 0) + 1
        out.append(best)
        left.remove(best)
    return out


ORDER = send_order()


def channel_tables():
    j = np.arange(256)
    p = np.arange(HALF)
    tables = []
    for odd in (0, 1):
        channel = (j // 4) * CPD + ((j // 2) % 2) * 2 + odd
        angle = 2.0 * np.pi * ((channel[:, None] * p[None, :]) % FRAME) / FRAME
        value = np.where((j % 2)[:, None] == 0, np.cos(angle), -np.sin(angle)) / math.sqrt(CH)
        tables.append(value.astype(np.float32))
    return np.concatenate(tables, axis=0)


def block_tables():
    n = np.arange(2 * SC)
    angle = 2.0 * np.pi * ((n[:, None] * n[None, :]) % (2 * SC)) / (2 * SC)
    factor = 1.0 / math.sqrt(2 * SC)
    return np.stack([np.cos(angle) * factor, np.sin(angle) * factor]).astype(np.float32)


def kernel(
    volt, taps, weights, ant_row, delay, chan_tab, blk_tab,
    out,
    vbuf, halo_a, wblk, wrow, chan, send_a, recv_a, perm, onehot, wstage, wperm,
    btmp, send_b, recv_b, chirp, fwd, inv, obuf,
    sem_v, sem_w, sem_ha, sem_hb, sa_send, sa_recv, sa_own, sb_send, sb_recv, sb_own, sem_o,
):
    sec = lax.axis_index("section")
    me = lax.axis_index("grp")
    y, z, x, c = me // (NZ * NX * NC), (me // (NX * NC)) % NZ, (me // NC) % NX, me % NC

    def partner(o):
        dy, dz, dx, dc = o
        return (((y + dy) % NY * NZ + (z + dz) % NZ) * NX + (x + dx) % NX) * NC + (c + dc) % NC

    barrier = pltpu.get_barrier_semaphore()
    for o in ORDER:
        pl.semaphore_signal(barrier, inc=1, device_id=(sec, partner(o)), device_id_type=MESH)
    pl.semaphore_signal(barrier, inc=1, device_id=(1 - sec, me), device_id_type=MESH)

    def load_v(i):
        t = CHUNKS - 1 - i
        return pltpu.make_async_copy(
            volt.at[:, pl.ds(pl.multiple_of(t * (SC * FRAME) - LEAD, 128), SC * FRAME + LEAD)],
            vbuf.at[lax.rem(i, 2)],
            sem_v.at[lax.rem(i, 2)],
        )

    def load_v0():
        return pltpu.make_async_copy(
            volt.at[:, pl.ds(0, SC * FRAME)],
            vbuf.at[(CHUNKS - 1) % 2, :, pl.ds(LEAD, SC * FRAME)],
            sem_v.at[(CHUNKS - 1) % 2],
        )

    def load_w(k):
        return pltpu.make_async_copy(
            weights.at[k // 2, lax.rem(k, 2)], wstage.at[lax.rem(k, 2)], sem_w.at[lax.rem(k, 2)]
        )

    load_v(0).start()
    load_w(0).start()

    row = lax.broadcasted_iota(jnp.int32, (256, 256), 0)
    col = lax.broadcasted_iota(jnp.int32, (256, 256), 1)
    perm[...] = jnp.where((row % 16) * 16 + row // 16 == col, 1.0, 0.0).astype(BF16)

    pl.semaphore_wait(barrier, NG)

    halo_copy = pltpu.make_async_remote_copy(
        volt.at[:, pl.ds(CHUNKS * SC * FRAME - LEAD, LEAD)],
        halo_a,
        sem_ha.at[0],
        sem_ha.at[1],
        device_id=(1 - sec, me),
        device_id_type=MESH,
    )

    @pl.when(sec == 0)
    def _():
        halo_copy.start()
        halo_a[...] = jnp.zeros_like(halo_a)
        recv_b[0] = jnp.zeros((2, ROWS, SC), BF16)

    def channelise(i, carry):
        t = CHUNKS - 1 - i
        slot = lax.rem(i, 2)

        @pl.when(i < CHUNKS - 2)
        def _():
            load_v(i + 1).start()

        @pl.when(i == CHUNKS - 2)
        def _():
            load_v0().start()

        @pl.when(i < CHUNKS - 1)
        def _():
            load_v(i).wait()

        @pl.when(i == CHUNKS - 1)
        def _():
            load_v0().wait()

            @pl.when(sec == 1)
            def _():
                halo_copy.wait_recv()

            vbuf[(CHUNKS - 1) % 2, :, pl.ds(0, LEAD)] = halo_a[...]

        def fir(sb, carry):
            base = pl.multiple_of(sb * (16 * FRAME), 16 * FRAME)
            for q in range(2):
                for s0 in (0, 8):
                    parts = []
                    for p0 in (q * 128, q * 128 + HALF):
                        frames = [
                            vbuf[slot, :, pl.ds(base + (s0 + f) * FRAME + p0, 128)].astype(F32)
                            for f in range(8 + TAPS - 1)
                        ]
                        tap = [taps[pl.ds(k, 1), pl.ds(p0, 128)] for k in range(TAPS)]
                        sums = []
                        for s in range(8):
                            acc = tap[0] * frames[s]
                            for k in range(1, TAPS):
                                acc = acc + tap[k] * frames[s + k]
                            sums.append(acc)
                        parts.append(sums)
                    for s in range(8):
                        lo, hi = parts[0][s], parts[1][s]
                        r0 = (s0 + s) * ANT
                        wblk[pl.ds(r0, ANT), pl.ds(q * 128, 128)] = (lo + hi).astype(BF16)
                        wblk[pl.ds(r0, ANT), pl.ds(HALF + q * 128, 128)] = (lo - hi).astype(BF16)
            moved = jnp.dot(perm[...], wblk[...], preferred_element_type=F32)
            wrow[:, pl.ds(pl.multiple_of(sb * 16, 16), 16), :] = moved.reshape(ANT, 16, FRAME).astype(BF16)
            return carry

        lax.fori_loop(0, SC // 16, fir, 0)

        def dft(ap, carry):
            rows = wrow[pl.ds(ap * 2, 2)].reshape(2 * SC, FRAME)
            for odd in range(2):
                res = lax.dot_general(
                    chan_tab[pl.ds(odd * 256, 256), :],
                    rows[:, odd * HALF : (odd + 1) * HALF],
                    (((1,), (1,)), ((), ())),
                    preferred_element_type=F32,
                ).astype(BF16)
                chan[odd, ap * 2] = res[:, :SC]
                chan[odd, ap * 2 + 1] = res[:, SC:]
            return carry

        lax.fori_loop(0, ANT // 2, dft, 0)

        def regroup(jh, carry):
            js = pl.ds(pl.multiple_of(jh * 16, 16), 16)
            both = jnp.concatenate(
                [chan[0, :, js, :].reshape(256, SC), chan[1, :, js, :].reshape(256, SC)], axis=1
            )
            moved = jnp.dot(perm[...], both, preferred_element_type=F32).astype(BF16)
            send_a[t, pl.ds(jh * 4, 4), pl.ds(0, 4)] = moved[:, :SC].reshape(4, 4, ANT, SC)
            send_a[t, pl.ds(jh * 4, 4), pl.ds(4, 4)] = moved[:, SC:].reshape(4, 4, ANT, SC)
            return carry

        lax.fori_loop(0, 16, regroup, 0)

        mine = pl.ds(pl.multiple_of(me * ANT, ANT), ANT)
        for o in ORDER:
            to = partner(o)
            pltpu.make_async_remote_copy(
                send_a.at[t, to],
                recv_a.at[t, :, mine, :],
                sa_send.at[t],
                sa_recv.at[t],
                device_id=(sec, to),
                device_id_type=MESH,
            ).start()
        pltpu.make_async_copy(send_a.at[t, me], recv_a.at[t, :, mine, :], sa_own.at[t]).start()
        return carry

    lax.fori_loop(0, CHUNKS, channelise, 0)

    def build_onehot(k, carry):
        r0 = pl.multiple_of(k * 128, 128)
        antenna = lax.broadcasted_iota(jnp.int32, (128, ALL_ANT), 0) + r0
        onehot[pl.ds(r0, 128), :] = jnp.where(antenna == ant_row[...], 1.0, 0.0).astype(BF16)
        return carry

    lax.fori_loop(0, ALL_ANT // 128, build_onehot, 0)

    def permute_weights(k, carry):
        @pl.when(k < 2 * CPD - 1)
        def _():
            load_w(k + 1).start()

        load_w(k).wait()

        def tile(n, carry):
            cols = pl.ds(pl.multiple_of(n * 256, 256), 256)
            wperm[k, :, cols] = jnp.dot(
                wstage[lax.rem(k, 2)], onehot[:, cols], preferred_element_type=F32
            ).astype(BF16)
            return carry

        lax.fori_loop(0, ALL_ANT // 256, tile, 0)
        return carry

    lax.fori_loop(0, 2 * CPD, permute_weights, 0)

    cos_t, sin_t = blk_tab[0], blk_tab[1]
    for h in range(2):
        part = slice(h * SC, (h + 1) * SC)
        fwd[pl.ds(h * 2 * SC, SC), pl.ds(0, 256)] = cos_t[part, :]
        fwd[pl.ds(h * 2 * SC, SC), pl.ds(256, 256)] = -sin_t[part, :]
        fwd[pl.ds(h * 2 * SC + SC, SC), pl.ds(0, 256)] = sin_t[part, :]
        fwd[pl.ds(h * 2 * SC + SC, SC), pl.ds(256, 256)] = cos_t[part, :]
    inv[pl.ds(0, 256), pl.ds(0, SC)] = cos_t[:, SC:]
    inv[pl.ds(0, 256), pl.ds(SC, SC)] = sin_t[:, SC:]
    inv[pl.ds(256, 256), pl.ds(0, SC)] = -sin_t[:, SC:]
    inv[pl.ds(256, 256), pl.ds(SC, SC)] = cos_t[:, SC:]

    def build_chirp(k, carry):
        r0 = pl.multiple_of(k * 64, 64)
        rows = lax.broadcasted_iota(jnp.int32, (64, 256), 0) + r0
        channel = (rows // BPD).astype(F32)
        stretch = 1.0 + channel / CH
        strength = 1.0 / (stretch * stretch * stretch)
        dl = jnp.concatenate([delay[...]] * 8, axis=0)
        dl = jnp.concatenate([dl, dl], axis=1)
        f = lax.broadcasted_iota(jnp.int32, (64, 256), 1)
        u = jnp.where(f < SC, f, f - 2 * SC).astype(F32)
        quarters = dl * strength * (u * u) * (1.0 / 32768.0)
        whole = jnp.round(quarters)
        a = (quarters - whole) * (math.pi / 2)
        k4 = (whole.astype(jnp.int32) - f) & 3
        a2 = a * a
        sin_a = a * (1.0 + a2 * (-1.0 / 6 + a2 * (1.0 / 120 + a2 * (-1.0 / 5040 + a2 * (1.0 / 362880)))))
        cos_a = 1.0 + a2 * (
            -0.5 + a2 * (1.0 / 24 + a2 * (-1.0 / 720 + a2 * (1.0 / 40320 + a2 * (-1.0 / 3628800))))
        )
        swap = (k4 & 1) == 1
        cos_p = jnp.where(swap, sin_a, cos_a)
        sin_p = jnp.where(swap, cos_a, sin_a)
        chirp[0, pl.ds(r0, 64), :] = jnp.where((k4 == 1) | (k4 == 2), -cos_p, cos_p)
        chirp[1, pl.ds(r0, 64), :] = jnp.where(k4 >= 2, -sin_p, sin_p)
        return carry

    lax.fori_loop(0, ROWS // 64, build_chirp, 0)

    def form(i, carry):
        t = CHUNKS - 1 - i
        own_rows = pl.ds(pl.multiple_of(me * ANT, ANT), ANT)
        got = recv_a.at[t, :, pl.ds(0, (NG - 1) * ANT), :]
        pltpu.make_async_remote_copy(
            got, got, sa_send.at[t], sa_recv.at[t], device_id=(sec, me), device_id_type=MESH
        ).wait_recv()
        pltpu.make_async_copy(send_a.at[t, me], recv_a.at[t, :, own_rows, :], sa_own.at[t]).wait()

        def pair(cp, carry):
            for cc in range(2):
                both = jnp.concatenate(
                    [recv_a[t, cc * 4 + cp * 2], recv_a[t, cc * 4 + cp * 2 + 1]], axis=1
                )
                w = cp * 4 + cc * 2
                for h in range(2):
                    bs = pl.ds(h * 256, 256)
                    by_real = jnp.dot(wperm[w, bs, :], both, preferred_element_type=F32)
                    by_imag = jnp.dot(wperm[w + 1, bs, :], both, preferred_element_type=F32)
                    btmp[cc, 0, bs, :] = by_real[:, :SC] - by_imag[:, SC:]
                    btmp[cc, 1, bs, :] = by_real[:, SC:] + by_imag[:, :SC]
            rs = pl.ds(pl.multiple_of(cp * 16, 16), 16)
            for ri in range(2):
                for h in range(4):
                    ds = pl.ds(h * 16, 16)
                    joined = jnp.concatenate(
                        [btmp[cc, ri, pl.ds(h * 128, 128), :].reshape(16, BPD, SC) for cc in range(2)],
                        axis=1,
                    )
                    send_b[t, ri, ds, rs, :] = joined.astype(BF16)
            return carry

        lax.fori_loop(0, CPD // 2, pair, 0)

        mine = pl.ds(pl.multiple_of(me * (CPD * BPD), CPD * BPD), CPD * BPD)
        for o in ORDER:
            to = partner(o)
            pltpu.make_async_remote_copy(
                send_b.at[t, :, to],
                recv_b.at[t + 1, :, mine, :],
                sb_send.at[t],
                sb_recv.at[t],
                device_id=(sec, to),
                device_id_type=MESH,
            ).start()
        pltpu.make_async_copy(send_b.at[t, :, me], recv_b.at[t + 1, :, mine, :], sb_own.at[t]).start()
        return carry

    lax.fori_loop(0, CHUNKS, form, 0)

    def wait_series(t):
        mine = pl.ds(pl.multiple_of(me * (CPD * BPD), CPD * BPD), CPD * BPD)
        got = recv_b.at[t + 1, :, pl.ds(0, (NG - 1) * CPD * BPD), :]
        pltpu.make_async_remote_copy(
            got, got, sb_send.at[t], sb_recv.at[t], device_id=(sec, me), device_id_type=MESH
        ).wait_recv()
        pltpu.make_async_copy(send_b.at[t, :, me], recv_b.at[t + 1, :, mine, :], sb_own.at[t]).wait()

    wait_series(CHUNKS - 1)
    halo_b = pltpu.make_async_remote_copy(
        recv_b.at[CHUNKS],
        recv_b.at[0],
        sem_hb.at[0],
        sem_hb.at[1],
        device_id=(1 - sec, me),
        device_id_type=MESH,
    )

    @pl.when(sec == 0)
    def _():
        halo_b.start()

    def store_out(m):
        return pltpu.make_async_copy(
            obuf.at[lax.rem(m, 2)],
            out.at[:, :, :, pl.ds(pl.multiple_of(m * SC, SC), SC)],
            sem_o.at[lax.rem(m, 2)],
        )

    def dedisperse(i, carry):
        m = CHUNKS - 1 - i

        @pl.when(m > 0)
        def _():
            wait_series(m - 1)

        @pl.when((m == 0) & (sec == 1))
        def _():
            halo_b.wait_recv()

        @pl.when(i >= 2)
        def _():
            store_out(m + 2).wait()

        def tile(r, carry):
            rs = pl.ds(pl.multiple_of(r * RT, RT), RT)
            block = jnp.concatenate(
                [recv_b[m, 0, rs, :], recv_b[m, 1, rs, :], recv_b[m + 1, 0, rs, :], recv_b[m + 1, 1, rs, :]],
                axis=1,
            )
            spec = jnp.dot(block, fwd[...], preferred_element_type=F32)
            sr, si = spec[:, :256], spec[:, 256:]
            cr, ci = chirp[0, rs, :], chirp[1, rs, :]
            filtered = jnp.concatenate(
                [(sr * cr - si * ci).astype(BF16), (sr * ci + si * cr).astype(BF16)], axis=1
            )
            res = jnp.dot(filtered, inv[...], preferred_element_type=F32)
            cs = pl.ds(pl.multiple_of(r * (RT // BPD), RT // BPD), RT // BPD)
            obuf[lax.rem(m, 2), cs, 0] = res[:, :SC].reshape(RT // BPD, BPD, SC)
            obuf[lax.rem(m, 2), cs, 1] = res[:, SC:].reshape(RT // BPD, BPD, SC)
            return carry

        lax.fori_loop(0, ROWS // RT, tile, 0)
        store_out(m).start()
        return carry

    lax.fori_loop(0, CHUNKS, dedisperse, 0)

    store_out(1).wait()
    store_out(0).wait()

    @pl.when(sec == 0)
    def _():
        halo_copy.wait_send()
        halo_b.wait_send()

    for t in range(CHUNKS):
        sent = send_a.at[t, pl.ds(0, NG - 1)]
        pltpu.make_async_remote_copy(
            sent, sent, sa_send.at[t], sa_recv.at[t], device_id=(sec, me), device_id_type=MESH
        ).wait_send()
        sent = send_b.at[t, :, pl.ds(0, NG - 1)]
        pltpu.make_async_remote_copy(
            sent, sent, sb_send.at[t], sb_recv.at[t], device_id=(sec, me), device_id_type=MESH
        ).wait_send()


def local(voltages, filter_taps, beam_weights, antenna_of_row, beam_delay):
    chan_tab = jnp.asarray(channel_tables()).astype(BF16)
    blk_tab = jnp.asarray(block_tables()).astype(BF16)
    ant_row = antenna_of_row.reshape(1, ALL_ANT)
    delay = jnp.broadcast_to(beam_delay.astype(F32)[:, None], (BPD, 128))
    vmem = pl.BlockSpec(memory_space=pltpu.VMEM)
    hbm = pl.BlockSpec(memory_space=pl.ANY)
    dma = pltpu.SemaphoreType.DMA
    return pl.pallas_call(
        kernel,
        out_shape=jax.ShapeDtypeStruct((CH, 2, BPD, CHUNKS * SC), F32),
        in_specs=[hbm, vmem, hbm, vmem, vmem, vmem, vmem],
        out_specs=hbm,
        scratch_shapes=[
            pltpu.VMEM((2, ANT, SC * FRAME + LEAD), BF16),
            pltpu.VMEM((ANT, LEAD), BF16),
            pltpu.VMEM((256, FRAME), BF16),
            pltpu.VMEM((ANT, SC, FRAME), BF16),
            pltpu.VMEM((2, ANT, 256, SC), BF16),
            pltpu.VMEM((CHUNKS, NG, 2 * CPD, ANT, SC), BF16),
            pltpu.VMEM((CHUNKS, 2 * CPD, ALL_ANT, SC), BF16),
            pltpu.VMEM((256, 256), BF16),
            pltpu.VMEM((ALL_ANT, ALL_ANT), BF16),
            pltpu.VMEM((2, BEAMS, ALL_ANT), BF16),
            pltpu.VMEM((2 * CPD, BEAMS, ALL_ANT), BF16),
            pltpu.VMEM((2, 2, BEAMS, SC), F32),
            pltpu.VMEM((CHUNKS, 2, NG, CPD * BPD, SC), BF16),
            pltpu.VMEM((CHUNKS + 1, 2, ROWS, SC), BF16),
            pltpu.VMEM((2, ROWS, 256), F32),
            pltpu.VMEM((512, 512), BF16),
            pltpu.VMEM((512, 256), BF16),
            pltpu.VMEM((2, CH, 2, BPD, SC), F32),
            dma((2,)), dma((2,)), dma((2,)), dma((2,)),
            dma((CHUNKS,)), dma((CHUNKS,)), dma((CHUNKS,)),
            dma((CHUNKS,)), dma((CHUNKS,)), dma((CHUNKS,)),
            dma((2,)),
        ],
        compiler_params=pltpu.CompilerParams(
            collective_id=0, has_side_effects=True, vmem_limit_bytes=67043328
        ),
    )(voltages, filter_taps, beam_weights, ant_row, delay, chan_tab, blk_tab)


def solution(mesh):
    in_specs = (P("grp", "section"), P(), P("grp", None, None, None), P(), P("grp"))
    out_specs = P(None, None, "grp", "section")
    return jax.shard_map(local, mesh=mesh, in_specs=in_specs, out_specs=out_specs, check_vma=False)
```

```python
import functools
import math
import random

import jax
import jax.numpy as jnp
import numpy as np
from jax import lax
from jax.experimental import pallas as pl
from jax.experimental.pallas import tpu as pltpu
from jax.sharding import PartitionSpec as P

MESH = pl.DeviceIdType.MESH
F32 = jnp.float32
BF16 = jnp.bfloat16
NG = 64
NY, NZ, NX, NC = 4, 4, 2, 2
ANT = 16
FRAME = 512
HALF = FRAME // 2
TAPS = 8
CH = 256
CPD = CH // NG
CHUNKS = 4
SC = 128
LEAD = (TAPS - 1) * FRAME
BEAMS = 512
BPD = BEAMS // NG
ROWS = CH * BPD
ALL_ANT = ANT * NG
HROWS = ROWS // 2
RT = 256
VMEM_LIMIT = 55 * 2**20


def send_order(seed=0):
    rng = random.Random(seed)
    left = [
        (dy, dz, dx, dc) for dy in range(NY) for dz in range(NZ) for dx in range(NX) for dc in range(NC)
    ][1:]
    rng.shuffle(left)
    load = {}

    def ports(o):
        p = []
        for name, d in (("y", o[0]), ("z", o[1])):
            if d in (1, 2):
                p.append(name + "+")
            if d in (2, 3):
                p.append(name + "-")
        if o[2]:
            p.append("x")
        return p

    out = []
    while left:
        best = min(
            left,
            key=lambda o: (max([load.get(p, 0) + 1 for p in ports(o)] + [0]), -len(ports(o)), rng.random()),
        )
        for p in ports(best):
            load[p] = load.get(p, 0) + 1
        out.append(best)
        left.remove(best)
    return out


ORDER = send_order()
CROSS = [o for o in ORDER if o[2]]


def channel_tables():
    j = np.arange(256)
    p = np.arange(HALF)
    tables = []
    for odd in (0, 1):
        channel = (j // 4) * CPD + ((j // 2) % 2) * 2 + odd
        angle = 2.0 * np.pi * ((channel[:, None] * p[None, :]) % FRAME) / FRAME
        value = np.where((j % 2)[:, None] == 0, np.cos(angle), -np.sin(angle)) / math.sqrt(CH)
        tables.append(value.astype(np.float32))
    return np.concatenate(tables, axis=0)


def block_tables():
    n = np.arange(2 * SC)
    angle = 2.0 * np.pi * ((n[:, None] * n[None, :]) % (2 * SC)) / (2 * SC)
    factor = 1.0 / math.sqrt(2 * SC)
    return np.stack([np.cos(angle) * factor, np.sin(angle) * factor]).astype(np.float32)


def kernel(
    volt, taps_h, weights, ant_row_h, delay, chan_tab_h, blk_tab_h,
    out,
    vbuf, halo_a, wblk, wrow, chan, send_a, recv_a, perm, onehot, wstage, wperm,
    btmp, send_b, recv_b, relay, chirp, fwd, inv, taps, ant_row, chan_tab, blk_tab,
    sem_v, sem_w, sem_t, sem_ha, sem_hb, sem_rl, sem_fw, sem_mc, sa_send, sa_recv, sb_send, sb_recv,
):
    sec = lax.axis_index("section")
    me = lax.axis_index("grp")
    y, z, x, c = me // (NZ * NX * NC), (me // (NX * NC)) % NZ, (me // NC) % NX, me % NC

    def partner(o):
        dy, dz, dx, dc = o
        return (((y + dy) % NY * NZ + (z + dz) % NZ) * NX + (x + dx) % NX) * NC + (c + dc) % NC

    def load_v(i):
        t = CHUNKS - 1 - i
        return pltpu.make_async_copy(
            volt.at[:, pl.ds(pl.multiple_of(t * (SC * FRAME) - LEAD, 128), SC * FRAME + LEAD)],
            vbuf.at[lax.rem(i, 2)],
            sem_v.at[lax.rem(i, 2)],
        )

    def load_v0():
        return pltpu.make_async_copy(
            volt.at[:, pl.ds(0, SC * FRAME)],
            vbuf.at[(CHUNKS - 1) % 2, :, pl.ds(LEAD, SC * FRAME)],
            sem_v.at[(CHUNKS - 1) % 2],
        )

    def load_w(k):
        return pltpu.make_async_copy(
            weights.at[k // 2, lax.rem(k, 2)], wstage.at[lax.rem(k, 2)], sem_w.at[lax.rem(k, 2)]
        )

    small = [
        pltpu.make_async_copy(src, dst, sem_t.at[n])
        for n, (src, dst) in enumerate(
            ((taps_h, taps), (chan_tab_h, chan_tab), (ant_row_h, ant_row), (blk_tab_h, blk_tab))
        )
    ]

    load_v(0).start()
    for copy in small:
        copy.start()
    load_w(0).start()
    barrier = pltpu.get_barrier_semaphore()
    for o in ORDER:
        pl.semaphore_signal(barrier, inc=1, device_id=(sec, partner(o)), device_id_type=MESH)
    for o in CROSS:
        pl.semaphore_signal(barrier, inc=1, device_id=(1 - sec, partner(o)), device_id_type=MESH)
    pl.semaphore_signal(barrier, inc=1, device_id=(1 - sec, me), device_id_type=MESH)

    row = lax.broadcasted_iota(jnp.int32, (256, 256), 0)
    col = lax.broadcasted_iota(jnp.int32, (256, 256), 1)
    perm[...] = jnp.where((row % 16) * 16 + row // 16 == col, 1.0, 0.0).astype(BF16)
    wblk[...] = jnp.zeros_like(wblk)
    small[0].wait()
    small[1].wait()

    halo_copy = pltpu.make_async_remote_copy(
        volt.at[:, pl.ds(CHUNKS * SC * FRAME - LEAD, LEAD)],
        halo_a,
        sem_ha.at[0],
        sem_ha.at[1],
        device_id=(1 - sec, me),
        device_id_type=MESH,
    )

    def fir_block(slot, sb, wslot):
        base = pl.multiple_of(sb * (16 * FRAME), 16 * FRAME)
        for q in range(2):
            for s0 in (0, 8):
                parts = []
                for p0 in (q * 128, q * 128 + HALF):
                    frames = [
                        vbuf[slot, :, pl.ds(base + (s0 + f) * FRAME + p0, 128)].astype(F32)
                        for f in range(8 + TAPS - 1)
                    ]
                    tap = [taps[pl.ds(k, 1), pl.ds(p0, 128)] for k in range(TAPS)]
                    sums = []
                    for s in range(8):
                        acc = tap[0] * frames[s]
                        for k in range(1, TAPS):
                            acc = acc + tap[k] * frames[s + k]
                        sums.append(acc)
                    parts.append(sums)
                for s in range(8):
                    lo, hi = parts[0][s], parts[1][s]
                    r0 = (s0 + s) * ANT
                    wblk[wslot, pl.ds(r0, ANT), pl.ds(q * 128, 128)] = (lo + hi).astype(BF16)
                    wblk[wslot, pl.ds(r0, ANT), pl.ds(HALF + q * 128, 128)] = (lo - hi).astype(BF16)

    def move_rows(wslot):
        return jnp.dot(perm[...], wblk[wslot], preferred_element_type=F32).reshape(ANT, 16, FRAME).astype(BF16)

    def channelise(i, carry):
        t = CHUNKS - 1 - i
        slot = lax.rem(i, 2)

        @pl.when(i < CHUNKS - 2)
        def _():
            load_v(i + 1).start()

        @pl.when(i == CHUNKS - 2)
        def _():
            load_v0().start()

        @pl.when(i < CHUNKS - 1)
        def _():
            load_v(i).wait()

        @pl.when(i == CHUNKS - 1)
        def _():
            load_v0().wait()

            @pl.when(sec == 1)
            def _():
                halo_copy.wait_recv()

            vbuf[(CHUNKS - 1) % 2, :, pl.ds(0, LEAD)] = halo_a[...]

        def fir(sb, carry):
            moved = move_rows(lax.rem(sb + 1, 2))
            fir_block(slot, sb, lax.rem(sb, 2))
            before = pl.multiple_of(jnp.maximum(sb - 1, 0) * 16, 16)
            wrow[:, pl.ds(before, 16), :] = moved
            return carry

        nblk = SC // 16
        lax.fori_loop(0, nblk, fir, 0)
        wrow[:, pl.ds((nblk - 1) * 16, 16), :] = move_rows((nblk - 1) % 2)

        def dft(ap2, carry):
            for u in range(2):
                ap = ap2 * 2 + u
                rows = wrow[pl.ds(ap * 2, 2)].reshape(2 * SC, FRAME)
                for odd in range(2):
                    res = lax.dot_general(
                        chan_tab[pl.ds(odd * 256, 256), :],
                        rows[:, odd * HALF : (odd + 1) * HALF],
                        (((1,), (1,)), ((), ())),
                        preferred_element_type=F32,
                    ).astype(BF16)
                    chan[odd, ap * 2] = res[:, :SC]
                    chan[odd, ap * 2 + 1] = res[:, SC:]
            return carry

        lax.fori_loop(0, ANT // 4, dft, 0)

        @pl.when(i == 0)
        def _():
            pl.semaphore_wait(barrier, NG + NG // 2)

        mine = pl.ds(pl.multiple_of(me * ANT, ANT), ANT)

        def shift(s):
            return s % NY, (s // NY + s % NY) % NZ

        def regroup(s):
            dy, dz = shift(s)
            jh = (y + dy) % NY * NZ + (z + dz) % NZ
            js = pl.ds(pl.multiple_of(jh * 16, 16), 16)
            both = jnp.concatenate(
                [chan[0, :, js, :].reshape(256, SC), chan[1, :, js, :].reshape(256, SC)], axis=1
            )
            moved = jnp.dot(perm[...], both, preferred_element_type=F32).astype(BF16)
            send_a[t, pl.ds(jh * 4, 4), pl.ds(0, 4)] = moved[:, :SC].reshape(4, 4, ANT, SC)
            send_a[t, pl.ds(jh * 4, 4), pl.ds(4, 4)] = moved[:, SC:].reshape(4, 4, ANT, SC)

        def send(s, pairs):
            dy, dz = shift(s)
            for dx, dc in pairs:
                to = partner((dy, dz, dx, dc))
                pltpu.make_async_remote_copy(
                    send_a.at[t, to],
                    recv_a.at[t, :, mine, :],
                    sa_send.at[t],
                    sa_recv.at[t],
                    device_id=(sec, to),
                    device_id_type=MESH,
                ).start()

        nshift = NY * NZ
        regroup(1)

        def step(k, carry):
            regroup(lax.rem(k + 2, nshift))
            send(k + 1, ((1, 0), (0, 1), (1, 1), (0, 0)))
            return carry

        lax.fori_loop(0, nshift - 1, step, 0)
        send(0, ((1, 0), (0, 1), (1, 1)))
        pltpu.make_async_copy(send_a.at[t, me], recv_a.at[t, :, mine, :], sa_recv.at[t]).start()

        @pl.when((i == 0) & (sec == 0))
        def _():
            halo_copy.start()
            halo_a[...] = jnp.zeros_like(halo_a)
            recv_b[0] = jnp.zeros((2, 2, NY * NZ, NX, 32, SC), BF16)

        return carry

    lax.fori_loop(0, CHUNKS - 1, channelise, 0)

    small[2].wait()

    def build_onehot(k, carry):
        r0 = pl.multiple_of(k * 128, 128)
        antenna = lax.broadcasted_iota(jnp.int32, (128, ALL_ANT), 0) + r0
        onehot[pl.ds(r0, 128), :] = jnp.where(antenna == ant_row[...], 1.0, 0.0).astype(BF16)
        return carry

    lax.fori_loop(0, ALL_ANT // 128, build_onehot, 0)

    def permute_weights(k, carry):
        @pl.when(k < 2 * CPD - 1)
        def _():
            load_w(k + 1).start()

        load_w(k).wait()

        def tile(n, carry):
            cols = pl.ds(pl.multiple_of(n * 256, 256), 256)
            wperm[k, :, cols] = jnp.dot(
                wstage[lax.rem(k, 2)], onehot[:, cols], preferred_element_type=F32
            ).astype(BF16)
            return carry

        lax.fori_loop(0, ALL_ANT // 256, tile, 0)
        return carry

    lax.fori_loop(0, 2 * CPD, permute_weights, 0)

    small[3].wait()
    cos_t, sin_t = blk_tab[0], blk_tab[1]
    for h in range(2):
        part = slice(h * SC, (h + 1) * SC)
        fwd[pl.ds(h * 2 * SC, SC), pl.ds(0, 256)] = cos_t[part, :]
        fwd[pl.ds(h * 2 * SC, SC), pl.ds(256, 256)] = -sin_t[part, :]
        fwd[pl.ds(h * 2 * SC + SC, SC), pl.ds(0, 256)] = sin_t[part, :]
        fwd[pl.ds(h * 2 * SC + SC, SC), pl.ds(256, 256)] = cos_t[part, :]
    inv[pl.ds(0, 256), pl.ds(0, SC)] = cos_t[:, SC:]
    inv[pl.ds(0, 256), pl.ds(SC, SC)] = sin_t[:, SC:]
    inv[pl.ds(256, 256), pl.ds(0, SC)] = -sin_t[:, SC:]
    inv[pl.ds(256, 256), pl.ds(SC, SC)] = cos_t[:, SC:]

    beam = lax.broadcasted_iota(jnp.int32, (BPD, 256), 0)
    dl8 = jnp.zeros((BPD, 256), F32)
    for b in range(BPD):
        dl8 = jnp.where(beam == b, delay[b].astype(F32), dl8)
    dl = jnp.concatenate([dl8] * 8, axis=0)

    def build_chirp(k, carry):
        half, r0 = k // (HROWS // 64), pl.multiple_of(lax.rem(k, HROWS // 64) * 64, 64)
        rows = lax.broadcasted_iota(jnp.int32, (64, 256), 0) + r0
        channel = (rows // 16 * CPD + half * 2 + (rows // BPD) % 2).astype(F32)
        stretch = 1.0 + channel / CH
        strength = 1.0 / (stretch * stretch * stretch)
        f = lax.broadcasted_iota(jnp.int32, (64, 256), 1)
        u = jnp.where(f < SC, f, f - 2 * SC).astype(F32)
        quarters = dl * strength * (u * u) * (1.0 / 32768.0)
        whole = jnp.round(quarters)
        a = (quarters - whole) * (math.pi / 2)
        k4 = (whole.astype(jnp.int32) - f) & 3
        a2 = a * a
        sin_a = a * (1.0 + a2 * (-1.0 / 6 + a2 * (1.0 / 120 + a2 * (-1.0 / 5040 + a2 * (1.0 / 362880)))))
        cos_a = 1.0 + a2 * (
            -0.5 + a2 * (1.0 / 24 + a2 * (-1.0 / 720 + a2 * (1.0 / 40320 + a2 * (-1.0 / 3628800))))
        )
        swap = (k4 & 1) == 1
        cos_p = jnp.where(swap, sin_a, cos_a)
        sin_p = jnp.where(swap, cos_a, sin_a)
        chirp[0, half, pl.ds(r0, 64), :] = jnp.where((k4 == 1) | (k4 == 2), -cos_p, cos_p)
        chirp[1, half, pl.ds(r0, 64), :] = jnp.where(k4 >= 2, -sin_p, sin_p)
        return carry

    lax.fori_loop(0, ROWS // 64, build_chirp, 0)

    own_b = pl.ds(pl.multiple_of(c * 16, 16), 16)
    yz = me // (NX * NC)

    def form(i, carry):
        t = CHUNKS - 1 - i
        got = recv_a.at[t]
        pltpu.make_async_remote_copy(
            got, got, sa_send.at[t], sa_recv.at[t], device_id=(sec, me), device_id_type=MESH
        ).wait_recv()

        def pair(cp, carry):
            for cc in range(2):
                both = jnp.concatenate(
                    [recv_a[t, cc * 4 + cp * 2], recv_a[t, cc * 4 + cp * 2 + 1]], axis=1
                )
                w = cp * 4 + cc * 2
                for h in range(2):
                    bs = pl.ds(h * 256, 256)
                    by_real = jnp.dot(wperm[w, bs, :], both, preferred_element_type=F32)
                    by_imag = jnp.dot(wperm[w + 1, bs, :], both, preferred_element_type=F32)
                    btmp[cc, 0, bs, :] = by_real[:, :SC] - by_imag[:, SC:]
                    btmp[cc, 1, bs, :] = by_real[:, SC:] + by_imag[:, :SC]
            for ri in range(2):
                for h in range(4):
                    joined = jnp.concatenate(
                        [btmp[cc, ri, pl.ds(h * 128, 128), :].reshape(16, BPD, SC) for cc in range(2)],
                        axis=1,
                    )
                    send_b[t, cp, ri, pl.ds(h * 16, 16)] = joined.astype(BF16)
            pltpu.make_async_copy(
                send_b.at[t, cp, :, me], recv_b.at[t + 1, cp, :, yz, x, own_b, :], sb_recv.at[t, cp]
            ).start()
            for o in ORDER:
                to = partner(o)
                pltpu.make_async_remote_copy(
                    send_b.at[t, cp, :, to],
                    recv_b.at[t + 1, cp, :, yz, x, own_b, :],
                    sb_send.at[t, cp],
                    sb_recv.at[t, cp],
                    device_id=(sec, to),
                    device_id_type=MESH,
                ).start()

            @pl.when((i == 0) & (sec == 0))
            def _():
                for o in CROSS:
                    to = partner(o)
                    pltpu.make_async_remote_copy(
                        send_b.at[CHUNKS - 1, cp, :, to],
                        recv_b.at[0, cp, :, yz, x, own_b, :],
                        sem_mc.at[0, cp],
                        sem_mc.at[1, cp],
                        device_id=(1 - sec, to),
                        device_id_type=MESH,
                    ).start()

            return carry

        lax.fori_loop(0, 2, pair, 0)
        return carry

    lax.fori_loop(0, 1, form, 0)
    lax.fori_loop(CHUNKS - 1, CHUNKS, channelise, 0)
    lax.fori_loop(1, CHUNKS - 1, form, 0)

    def wait_series(t, cp):
        got = recv_b.at[t + 1, cp]
        pltpu.make_async_remote_copy(
            got, got, sb_send.at[t, cp], sb_recv.at[t, cp], device_id=(sec, me), device_id_type=MESH
        ).wait_recv()

    flip = partner((0, 0, 1, 0))
    wait_series(CHUNKS - 1, 0)
    wait_series(CHUNKS - 1, 1)
    halo_b = pltpu.make_async_remote_copy(
        recv_b.at[CHUNKS, 0, :, :, x],
        recv_b.at[0, 0, :, :, x],
        sem_hb.at[0],
        sem_hb.at[1],
        device_id=(1 - sec, me),
        device_id_type=MESH,
    )
    to_relay = pltpu.make_async_remote_copy(
        recv_b.at[CHUNKS, 1, :, :, x],
        relay,
        sem_rl.at[0],
        sem_rl.at[1],
        device_id=(1 - sec, flip),
        device_id_type=MESH,
    )
    forward = pltpu.make_async_remote_copy(
        relay,
        recv_b.at[0, 1, :, :, 1 - x],
        sem_fw.at[0],
        sem_fw.at[1],
        device_id=(sec, flip),
        device_id_type=MESH,
    )

    @pl.when(sec == 0)
    def _():
        to_relay.start()
        halo_b.start()

    lax.fori_loop(CHUNKS - 1, CHUNKS, form, 0)

    @pl.when(sec == 1)
    def _():
        to_relay.wait_recv()
        forward.start()

    def dedisperse(n, carry):
        late = n // 4
        m = (1 - late) * (3 - n // 2) + late * (1 - n % 2)
        cp = (1 - late) * (n % 2) + late * ((n // 2) % 2)

        @pl.when(m > 0)
        def _():
            wait_series(m - 1, cp)

        @pl.when((n == 5) & (sec == 1))
        def _():
            halo_b.wait_recv()
            pltpu.make_async_remote_copy(
                relay, recv_b.at[0, 1, :, :, x], sem_fw.at[0], sem_fw.at[1],
                device_id=(sec, flip), device_id_type=MESH,
            ).wait_recv()
            for half in range(2):
                got = recv_b.at[0, half, :, :, 1 - x]
                pltpu.make_async_remote_copy(
                    got, got, sem_mc.at[0, half], sem_mc.at[1, half],
                    device_id=(sec, flip), device_id_type=MESH,
                ).wait_recv()

        def tile(r, carry):
            rs = pl.ds(pl.multiple_of(r * RT, RT), RT)
            qs = pl.ds(r * (RT // 64), RT // 64)
            block = jnp.concatenate(
                [recv_b[m + d, cp, ri, qs].reshape(RT, SC) for d in range(2) for ri in range(2)], axis=1
            )
            spec = jnp.dot(block, fwd[...], preferred_element_type=F32)
            sr, si = spec[:, :256], spec[:, 256:]
            cr, ci = chirp[0, cp, rs, :], chirp[1, cp, rs, :]
            filtered = jnp.concatenate(
                [(sr * cr - si * ci).astype(BF16), (sr * ci + si * cr).astype(BF16)], axis=1
            )
            res = jnp.dot(filtered, inv[...], preferred_element_type=F32)
            gs = pl.ds(r * (RT // 16), RT // 16)
            ns = pl.ds(pl.multiple_of(m * SC, SC), SC)
            for ri in range(2):
                part = res[:, ri * SC : (ri + 1) * SC].reshape(RT // 16, 2, BPD, SC)
                for cc in range(2):
                    out[gs, cp * 2 + cc, ri, :, ns] = part[:, cc]
            return carry

        lax.fori_loop(0, HROWS // RT, tile, 0)
        return carry

    lax.fori_loop(0, 2 * CHUNKS, dedisperse, 0)

    @pl.when(sec == 0)
    def _():
        halo_copy.wait_send()
        halo_b.wait_send()
        to_relay.wait_send()
        for half in range(2):
            sent = send_b.at[CHUNKS - 1, half, :, pl.ds(0, NG // 2)]
            pltpu.make_async_remote_copy(
                sent, sent, sem_mc.at[0, half], sem_mc.at[1, half],
                device_id=(1 - sec, me), device_id_type=MESH,
            ).wait_send()

    @pl.when(sec == 1)
    def _():
        forward.wait_send()

    for t in range(CHUNKS):
        sent = send_a.at[t, pl.ds(0, NG - 1)]
        pltpu.make_async_remote_copy(
            sent, sent, sa_send.at[t], sa_recv.at[t], device_id=(sec, me), device_id_type=MESH
        ).wait_send()
        for cp in range(2):
            sent = send_b.at[t, cp, :, pl.ds(0, NG - 1)]
            pltpu.make_async_remote_copy(
                sent, sent, sb_send.at[t, cp], sb_recv.at[t, cp], device_id=(sec, me), device_id_type=MESH
            ).wait_send()


def local(voltages, filter_taps, beam_weights, antenna_of_row, beam_delay):
    chan_tab = jnp.asarray(channel_tables()).astype(BF16)
    blk_tab = jnp.asarray(block_tables()).astype(BF16)
    ant_row = antenna_of_row.reshape(1, ALL_ANT)
    vmem = pl.BlockSpec(memory_space=pltpu.VMEM)
    smem = pl.BlockSpec(memory_space=pltpu.SMEM)
    hbm = pl.BlockSpec(memory_space=pl.ANY)
    dma = pltpu.SemaphoreType.DMA
    series = pl.pallas_call(
        kernel,
        out_shape=pltpu.VMEM((NG, CPD, 2, BPD, CHUNKS * SC), F32),
        in_specs=[hbm, hbm, hbm, hbm, smem, hbm, hbm],
        out_specs=vmem,
        scratch_shapes=[
            pltpu.VMEM((2, ANT, SC * FRAME + LEAD), BF16),
            pltpu.VMEM((ANT, LEAD), BF16),
            pltpu.VMEM((2, 256, FRAME), BF16),
            pltpu.VMEM((ANT, SC, FRAME), BF16),
            pltpu.VMEM((2, ANT, 256, SC), BF16),
            pltpu.VMEM((CHUNKS, NG, 2 * CPD, ANT, SC), BF16),
            pltpu.VMEM((CHUNKS, 2 * CPD, ALL_ANT, SC), BF16),
            pltpu.VMEM((256, 256), BF16),
            pltpu.VMEM((ALL_ANT, ALL_ANT), BF16),
            pltpu.VMEM((2, BEAMS, ALL_ANT), BF16),
            pltpu.VMEM((2 * CPD, BEAMS, ALL_ANT), BF16),
            pltpu.VMEM((2, 2, BEAMS, SC), F32),
            pltpu.VMEM((CHUNKS, 2, 2, NG, 16, SC), BF16),
            pltpu.VMEM((CHUNKS + 1, 2, 2, NY * NZ, NX, 32, SC), BF16),
            pltpu.VMEM((2, NY * NZ, 32, SC), BF16),
            pltpu.VMEM((2, 2, HROWS, 256), F32),
            pltpu.VMEM((512, 512), BF16),
            pltpu.VMEM((512, 256), BF16),
            pltpu.VMEM((TAPS, FRAME), F32),
            pltpu.VMEM((1, ALL_ANT), jnp.int32),
            pltpu.VMEM((512, HALF), BF16),
            pltpu.VMEM((2, 256, 256), BF16),
            dma((2,)), dma((2,)), dma((4,)), dma((2,)), dma((2,)), dma((2,)), dma((2,)), dma((2, 2)),
            dma((CHUNKS,)), dma((CHUNKS,)), dma((CHUNKS, 2)), dma((CHUNKS, 2)),
        ],
        compiler_params=pltpu.CompilerParams(
            collective_id=0, has_side_effects=True, vmem_limit_bytes=VMEM_LIMIT
        ),
    )(voltages, filter_taps, beam_weights, ant_row, beam_delay, chan_tab, blk_tab)
    return series.reshape(CH, 2, BPD, CHUNKS * SC)


def solution(mesh):
    in_specs = (P("grp", "section"), P(), P("grp", None, None, None), P(), P("grp"))
    out_specs = P(None, None, "grp", "section")
    return jax.shard_map(local, mesh=mesh, in_specs=in_specs, out_specs=out_specs, check_vma=False)
```

```python
import functools
import math
import random

import jax
import jax.numpy as jnp
import numpy as np
from jax import lax
from jax.experimental import pallas as pl
from jax.experimental.pallas import tpu as pltpu
from jax.sharding import PartitionSpec as P

MESH = pl.DeviceIdType.MESH
F32 = jnp.float32
BF16 = jnp.bfloat16
NG = 64
NY, NZ, NX, NC = 4, 4, 2, 2
ANT = 16
FRAME = 512
HALF = FRAME // 2
TAPS = 8
CH = 256
CPD = CH // NG
CHUNKS = 4
SC = 128
LEAD = (TAPS - 1) * FRAME
BEAMS = 512
BPD = BEAMS // NG
ROWS = CH * BPD
ALL_ANT = ANT * NG
HROWS = ROWS // 2
RT = 256
VMEM_LIMIT = 55 * 2**20


def send_order(seed=0):
    rng = random.Random(seed)
    left = [
        (dy, dz, dx, dc) for dy in range(NY) for dz in range(NZ) for dx in range(NX) for dc in range(NC)
    ][1:]
    rng.shuffle(left)
    load = {}

    def ports(o):
        p = []
        for name, d in (("y", o[0]), ("z", o[1])):
            if d in (1, 2):
                p.append(name + "+")
            if d in (2, 3):
                p.append(name + "-")
        if o[2]:
            p.append("x")
        return p

    out = []
    while left:
        best = min(
            left,
            key=lambda o: (max([load.get(p, 0) + 1 for p in ports(o)] + [0]), -len(ports(o)), rng.random()),
        )
        for p in ports(best):
            load[p] = load.get(p, 0) + 1
        out.append(best)
        left.remove(best)
    return out


ORDER = send_order()
CROSS = [o for o in ORDER if o[2]]


def channel_tables():
    j = np.arange(256)
    p = np.arange(HALF)
    tables = []
    for odd in (0, 1):
        channel = (j // 4) * CPD + ((j // 2) % 2) * 2 + odd
        angle = 2.0 * np.pi * ((channel[:, None] * p[None, :]) % FRAME) / FRAME
        value = np.where((j % 2)[:, None] == 0, np.cos(angle), -np.sin(angle)) / math.sqrt(CH)
        tables.append(value.astype(np.float32))
    return np.concatenate(tables, axis=0)


def block_tables():
    n = np.arange(2 * SC)
    angle = 2.0 * np.pi * ((n[:, None] * n[None, :]) % (2 * SC)) / (2 * SC)
    factor = 1.0 / math.sqrt(2 * SC)
    return np.stack([np.cos(angle) * factor, np.sin(angle) * factor]).astype(np.float32)


def kernel(
    volt, taps_h, weights, ant_row_h, delay, chan_tab_h, blk_tab_h,
    out,
    vbuf, halo_a, wblk, wrow, chan, send_a, recv_a, perm, onehot, wstage, wperm,
    btmp, send_b, recv_b, relay, chirp, fwd, inv, taps, ant_row, chan_tab, blk_tab,
    sem_v, sem_w, sem_t, sem_ha, sem_hb, sem_rl, sem_fw, sem_mc, sa_send, sa_recv, sb_send, sb_recv,
):
    sec = lax.axis_index("section")
    me = lax.axis_index("grp")
    y, z, x, c = me // (NZ * NX * NC), (me // (NX * NC)) % NZ, (me // NC) % NX, me % NC

    def partner(o):
        dy, dz, dx, dc = o
        return (((y + dy) % NY * NZ + (z + dz) % NZ) * NX + (x + dx) % NX) * NC + (c + dc) % NC

    def load_v(i):
        t = CHUNKS - 1 - i
        return pltpu.make_async_copy(
            volt.at[:, pl.ds(pl.multiple_of(t * (SC * FRAME) - LEAD, 128), SC * FRAME + LEAD)],
            vbuf.at[lax.rem(i, 2)],
            sem_v.at[lax.rem(i, 2)],
        )

    def load_v0():
        return pltpu.make_async_copy(
            volt.at[:, pl.ds(0, SC * FRAME)],
            vbuf.at[(CHUNKS - 1) % 2, :, pl.ds(LEAD, SC * FRAME)],
            sem_v.at[(CHUNKS - 1) % 2],
        )

    def load_w(k):
        return pltpu.make_async_copy(
            weights.at[k // 2, lax.rem(k, 2)], wstage.at[lax.rem(k, 2)], sem_w.at[lax.rem(k, 2)]
        )

    small = [
        pltpu.make_async_copy(src, dst, sem_t.at[n])
        for n, (src, dst) in enumerate(
            ((taps_h, taps), (chan_tab_h, chan_tab), (ant_row_h, ant_row), (blk_tab_h, blk_tab))
        )
    ]

    load_v(0).start()
    for copy in small:
        copy.start()
    load_w(0).start()
    barrier = pltpu.get_barrier_semaphore()
    for o in ORDER:
        pl.semaphore_signal(barrier, inc=1, device_id=(sec, partner(o)), device_id_type=MESH)
    for o in CROSS:
        pl.semaphore_signal(barrier, inc=1, device_id=(1 - sec, partner(o)), device_id_type=MESH)
    pl.semaphore_signal(barrier, inc=1, device_id=(1 - sec, me), device_id_type=MESH)

    row = lax.broadcasted_iota(jnp.int32, (256, 256), 0)
    col = lax.broadcasted_iota(jnp.int32, (256, 256), 1)
    perm[...] = jnp.where((row % 16) * 16 + row // 16 == col, 1.0, 0.0).astype(BF16)
    wblk[...] = jnp.zeros_like(wblk)
    small[0].wait()
    small[1].wait()

    halo_copy = pltpu.make_async_remote_copy(
        volt.at[:, pl.ds(CHUNKS * SC * FRAME - LEAD, LEAD)],
        halo_a,
        sem_ha.at[0],
        sem_ha.at[1],
        device_id=(1 - sec, me),
        device_id_type=MESH,
    )

    def fir_block(slot, sb, wslot):
        base = pl.multiple_of(sb * (16 * FRAME), 16 * FRAME)
        for q in range(2):
            for s0 in (0, 8):
                parts = []
                for p0 in (q * 128, q * 128 + HALF):
                    frames = [
                        vbuf[slot, :, pl.ds(base + (s0 + f) * FRAME + p0, 128)].astype(F32)
                        for f in range(8 + TAPS - 1)
                    ]
                    tap = [taps[pl.ds(k, 1), pl.ds(p0, 128)] for k in range(TAPS)]
                    sums = []
                    for s in range(8):
                        acc = tap[0] * frames[s]
                        for k in range(1, TAPS):
                            acc = acc + tap[k] * frames[s + k]
                        sums.append(acc)
                    parts.append(sums)
                for s in range(8):
                    lo, hi = parts[0][s], parts[1][s]
                    r0 = (s0 + s) * ANT
                    wblk[wslot, pl.ds(r0, ANT), pl.ds(q * 128, 128)] = (lo + hi).astype(BF16)
                    wblk[wslot, pl.ds(r0, ANT), pl.ds(HALF + q * 128, 128)] = (lo - hi).astype(BF16)

    def move_rows(wslot):
        return jnp.dot(perm[...], wblk[wslot], preferred_element_type=F32).reshape(ANT, 16, FRAME).astype(BF16)

    def channelise(i, carry):
        t = CHUNKS - 1 - i
        slot = lax.rem(i, 2)

        @pl.when(i < CHUNKS - 2)
        def _():
            load_v(i + 1).start()

        @pl.when(i == CHUNKS - 2)
        def _():
            load_v0().start()

        @pl.when(i < CHUNKS - 1)
        def _():
            load_v(i).wait()

        @pl.when(i == CHUNKS - 1)
        def _():
            load_v0().wait()

            @pl.when(sec == 1)
            def _():
                halo_copy.wait_recv()

            vbuf[(CHUNKS - 1) % 2, :, pl.ds(0, LEAD)] = halo_a[...]

        def fir(sb, carry):
            moved = move_rows(lax.rem(sb + 1, 2))
            fir_block(slot, sb, lax.rem(sb, 2))
            before = pl.multiple_of(jnp.maximum(sb - 1, 0) * 16, 16)
            wrow[:, pl.ds(before, 16), :] = moved
            return carry

        nblk = SC // 16
        lax.fori_loop(0, nblk, fir, 0)
        wrow[:, pl.ds((nblk - 1) * 16, 16), :] = move_rows((nblk - 1) % 2)

        def dft(ap2, carry):
            for u in range(2):
                ap = ap2 * 2 + u
                rows = wrow[pl.ds(ap * 2, 2)].reshape(2 * SC, FRAME)
                for odd in range(2):
                    res = lax.dot_general(
                        chan_tab[pl.ds(odd * 256, 256), :],
                        rows[:, odd * HALF : (odd + 1) * HALF],
                        (((1,), (1,)), ((), ())),
                        preferred_element_type=F32,
                    ).astype(BF16)
                    chan[odd, ap * 2] = res[:, :SC]
                    chan[odd, ap * 2 + 1] = res[:, SC:]
            return carry

        lax.fori_loop(0, ANT // 4, dft, 0)

        @pl.when(i == 0)
        def _():
            pl.semaphore_wait(barrier, NG + NG // 2)

        mine = pl.ds(pl.multiple_of(me * ANT, ANT), ANT)

        def shift(s):
            return s % NY, (s // NY + s % NY) % NZ

        def regroup(s):
            dy, dz = shift(s)
            jh = (y + dy) % NY * NZ + (z + dz) % NZ
            js = pl.ds(pl.multiple_of(jh * 16, 16), 16)
            both = jnp.concatenate(
                [chan[0, :, js, :].reshape(256, SC), chan[1, :, js, :].reshape(256, SC)], axis=1
            )
            moved = jnp.dot(perm[...], both, preferred_element_type=F32).astype(BF16)
            send_a[t, pl.ds(jh * 4, 4), pl.ds(0, 4)] = moved[:, :SC].reshape(4, 4, ANT, SC)
            send_a[t, pl.ds(jh * 4, 4), pl.ds(4, 4)] = moved[:, SC:].reshape(4, 4, ANT, SC)

        def send(s, r):
            dy, dz = shift(s)
            q = (2 * s + s // NY + r) % (NX * NC)
            to = partner((dy, dz, q // NC, q % NC))
            pltpu.make_async_remote_copy(
                send_a.at[t, to],
                recv_a.at[t, :, mine, :],
                sa_send.at[t],
                sa_recv.at[t],
                device_id=(sec, to),
                device_id_type=MESH,
            ).start()

        nshift = NY * NZ
        regroup(1)

        def step(k, carry):
            regroup(lax.rem(k + 2, nshift))
            send(k + 1, 0)
            return carry

        lax.fori_loop(0, nshift - 1, step, 0)
        pltpu.make_async_copy(send_a.at[t, me], recv_a.at[t, :, mine, :], sa_recv.at[t]).start()

        def rest(r, carry):
            for k in range(nshift):
                send((k + 1) % nshift, r)
            return carry

        lax.fori_loop(1, NX * NC, rest, 0)

        @pl.when((i == 0) & (sec == 0))
        def _():
            halo_copy.start()
            halo_a[...] = jnp.zeros_like(halo_a)
            recv_b[0] = jnp.zeros((2, 2, NY * NZ, NX, 32, SC), BF16)

        return carry

    lax.fori_loop(0, CHUNKS - 1, channelise, 0)

    small[2].wait()

    def build_onehot(k, carry):
        r0 = pl.multiple_of(k * 128, 128)
        antenna = lax.broadcasted_iota(jnp.int32, (128, ALL_ANT), 0) + r0
        onehot[pl.ds(r0, 128), :] = jnp.where(antenna == ant_row[...], 1.0, 0.0).astype(BF16)
        return carry

    lax.fori_loop(0, ALL_ANT // 128, build_onehot, 0)

    def permute_weights(k, carry):
        @pl.when(k < 2 * CPD - 1)
        def _():
            load_w(k + 1).start()

        load_w(k).wait()

        def tile(n, carry):
            cols = pl.ds(pl.multiple_of(n * 256, 256), 256)
            wperm[k, :, cols] = jnp.dot(
                wstage[lax.rem(k, 2)], onehot[:, cols], preferred_element_type=F32
            ).astype(BF16)
            return carry

        lax.fori_loop(0, ALL_ANT // 256, tile, 0)
        return carry

    lax.fori_loop(0, 2 * CPD, permute_weights, 0)

    small[3].wait()
    cos_t, sin_t = blk_tab[0], blk_tab[1]
    for h in range(2):
        part = slice(h * SC, (h + 1) * SC)
        fwd[pl.ds(h * 2 * SC, SC), pl.ds(0, 256)] = cos_t[part, :]
        fwd[pl.ds(h * 2 * SC, SC), pl.ds(256, 256)] = -sin_t[part, :]
        fwd[pl.ds(h * 2 * SC + SC, SC), pl.ds(0, 256)] = sin_t[part, :]
        fwd[pl.ds(h * 2 * SC + SC, SC), pl.ds(256, 256)] = cos_t[part, :]
    inv[pl.ds(0, 256), pl.ds(0, SC)] = cos_t[:, SC:]
    inv[pl.ds(0, 256), pl.ds(SC, SC)] = sin_t[:, SC:]
    inv[pl.ds(256, 256), pl.ds(0, SC)] = -sin_t[:, SC:]
    inv[pl.ds(256, 256), pl.ds(SC, SC)] = cos_t[:, SC:]

    beam = lax.broadcasted_iota(jnp.int32, (BPD, 256), 0)
    dl8 = jnp.zeros((BPD, 256), F32)
    for b in range(BPD):
        dl8 = jnp.where(beam == b, delay[b].astype(F32), dl8)
    dl = jnp.concatenate([dl8] * 8, axis=0)

    def build_chirp(k, carry):
        half, r0 = k // (HROWS // 64), pl.multiple_of(lax.rem(k, HROWS // 64) * 64, 64)
        rows = lax.broadcasted_iota(jnp.int32, (64, 256), 0) + r0
        channel = (rows // 16 * CPD + half * 2 + (rows // BPD) % 2).astype(F32)
        stretch = 1.0 + channel / CH
        strength = 1.0 / (stretch * stretch * stretch)
        f = lax.broadcasted_iota(jnp.int32, (64, 256), 1)
        u = jnp.where(f < SC, f, f - 2 * SC).astype(F32)
        quarters = dl * strength * (u * u) * (1.0 / 32768.0)
        whole = jnp.round(quarters)
        a = (quarters - whole) * (math.pi / 2)
        k4 = (whole.astype(jnp.int32) - f) & 3
        a2 = a * a
        sin_a = a * (1.0 + a2 * (-1.0 / 6 + a2 * (1.0 / 120 + a2 * (-1.0 / 5040 + a2 * (1.0 / 362880)))))
        cos_a = 1.0 + a2 * (
            -0.5 + a2 * (1.0 / 24 + a2 * (-1.0 / 720 + a2 * (1.0 / 40320 + a2 * (-1.0 / 3628800))))
        )
        swap = (k4 & 1) == 1
        cos_p = jnp.where(swap, sin_a, cos_a)
        sin_p = jnp.where(swap, cos_a, sin_a)
        chirp[0, half, pl.ds(r0, 64), :] = jnp.where((k4 == 1) | (k4 == 2), -cos_p, cos_p)
        chirp[1, half, pl.ds(r0, 64), :] = jnp.where(k4 >= 2, -sin_p, sin_p)
        return carry

    lax.fori_loop(0, ROWS // 64, build_chirp, 0)

    own_b = pl.ds(pl.multiple_of(c * 16, 16), 16)
    yz = me // (NX * NC)

    def form(i, carry):
        t = CHUNKS - 1 - i
        got = recv_a.at[t]
        pltpu.make_async_remote_copy(
            got, got, sa_send.at[t], sa_recv.at[t], device_id=(sec, me), device_id_type=MESH
        ).wait_recv()

        def pair(cp, carry):
            for cc in range(2):
                both = jnp.concatenate(
                    [recv_a[t, cc * 4 + cp * 2], recv_a[t, cc * 4 + cp * 2 + 1]], axis=1
                )
                w = cp * 4 + cc * 2
                for h in range(2):
                    bs = pl.ds(h * 256, 256)
                    by_real = jnp.dot(wperm[w, bs, :], both, preferred_element_type=F32)
                    by_imag = jnp.dot(wperm[w + 1, bs, :], both, preferred_element_type=F32)
                    btmp[cc, 0, bs, :] = by_real[:, :SC] - by_imag[:, SC:]
                    btmp[cc, 1, bs, :] = by_real[:, SC:] + by_imag[:, :SC]
            for ri in range(2):
                for h in range(4):
                    joined = jnp.concatenate(
                        [btmp[cc, ri, pl.ds(h * 128, 128), :].reshape(16, BPD, SC) for cc in range(2)],
                        axis=1,
                    )
                    send_b[t, cp, ri, pl.ds(h * 16, 16)] = joined.astype(BF16)
            pltpu.make_async_copy(
                send_b.at[t, cp, :, me], recv_b.at[t + 1, cp, :, yz, x, own_b, :], sb_recv.at[t, cp]
            ).start()
            for o in ORDER:
                to = partner(o)
                pltpu.make_async_remote_copy(
                    send_b.at[t, cp, :, to],
                    recv_b.at[t + 1, cp, :, yz, x, own_b, :],
                    sb_send.at[t, cp],
                    sb_recv.at[t, cp],
                    device_id=(sec, to),
                    device_id_type=MESH,
                ).start()

            @pl.when((i == 0) & (sec == 0))
            def _():
                for o in CROSS:
                    to = partner(o)
                    pltpu.make_async_remote_copy(
                        send_b.at[CHUNKS - 1, cp, :, to],
                        recv_b.at[0, cp, :, yz, x, own_b, :],
                        sem_mc.at[0, cp],
                        sem_mc.at[1, cp],
                        device_id=(1 - sec, to),
                        device_id_type=MESH,
                    ).start()

            return carry

        lax.fori_loop(0, 2, pair, 0)
        return carry

    lax.fori_loop(0, 1, form, 0)
    lax.fori_loop(CHUNKS - 1, CHUNKS, channelise, 0)
    lax.fori_loop(1, CHUNKS - 1, form, 0)

    def wait_series(t, cp):
        got = recv_b.at[t + 1, cp]
        pltpu.make_async_remote_copy(
            got, got, sb_send.at[t, cp], sb_recv.at[t, cp], device_id=(sec, me), device_id_type=MESH
        ).wait_recv()

    flip = partner((0, 0, 1, 0))
    wait_series(CHUNKS - 1, 0)
    wait_series(CHUNKS - 1, 1)
    halo_b = pltpu.make_async_remote_copy(
        recv_b.at[CHUNKS, 0, :, :, x],
        recv_b.at[0, 0, :, :, x],
        sem_hb.at[0],
        sem_hb.at[1],
        device_id=(1 - sec, me),
        device_id_type=MESH,
    )
    to_relay = pltpu.make_async_remote_copy(
        recv_b.at[CHUNKS, 1, :, :, x],
        relay,
        sem_rl.at[0],
        sem_rl.at[1],
        device_id=(1 - sec, flip),
        device_id_type=MESH,
    )
    forward = pltpu.make_async_remote_copy(
        relay,
        recv_b.at[0, 1, :, :, 1 - x],
        sem_fw.at[0],
        sem_fw.at[1],
        device_id=(sec, flip),
        device_id_type=MESH,
    )

    @pl.when(sec == 0)
    def _():
        to_relay.start()
        halo_b.start()

    @pl.when(sec == 1)
    def _():
        to_relay.wait_recv()
        forward.start()

    lax.fori_loop(CHUNKS - 1, CHUNKS, form, 0)

    def series_rows(slot, cp, r):
        qs = pl.ds(r * (RT // 64), RT // 64)
        return [recv_b[slot, cp, ri, qs].reshape(RT, SC) for ri in range(2)]

    def finish(m, cp, r, spec):
        rs = pl.ds(pl.multiple_of(r * RT, RT), RT)
        sr, si = spec[:, :256], spec[:, 256:]
        cr, ci = chirp[0, cp, rs, :], chirp[1, cp, rs, :]
        filtered = jnp.concatenate(
            [(sr * cr - si * ci).astype(BF16), (sr * ci + si * cr).astype(BF16)], axis=1
        )
        res = jnp.dot(filtered, inv[...], preferred_element_type=F32)
        gs = pl.ds(r * (RT // 16), RT // 16)
        ns = pl.ds(pl.multiple_of(m * SC, SC), SC)
        for ri in range(2):
            part = res[:, ri * SC : (ri + 1) * SC].reshape(RT // 16, 2, BPD, SC)
            for cc in range(2):
                out[gs, cp * 2 + cc, ri, :, ns] = part[:, cc]

    def early(n, carry):
        m, cp = 3 - n // 2, n % 2
        wait_series(m - 1, cp)

        def tile(r, carry):
            block = jnp.concatenate(series_rows(m, cp, r) + series_rows(m + 1, cp, r), axis=1)
            finish(m, cp, r, jnp.dot(block, fwd[...], preferred_element_type=F32))
            return carry

        lax.fori_loop(0, HROWS // RT, tile, 0)
        return carry

    lax.fori_loop(0, 4, early, 0)

    def partial(k, carry):
        cp, halo = k % 2, k // 2

        @pl.when((k == 2) & (sec == 1))
        def _():
            halo_b.wait_recv()
            pltpu.make_async_remote_copy(
                relay, recv_b.at[0, 1, :, :, x], sem_fw.at[0], sem_fw.at[1],
                device_id=(sec, flip), device_id_type=MESH,
            ).wait_recv()
            for half in range(2):
                got = recv_b.at[0, half, :, :, 1 - x]
                pltpu.make_async_remote_copy(
                    got, got, sem_mc.at[0, half], sem_mc.at[1, half],
                    device_id=(sec, flip), device_id_type=MESH,
                ).wait_recv()

        slot = 2 * (1 - halo)
        table = pl.ds(pl.multiple_of((1 - halo) * 2 * SC, 2 * SC), 2 * SC)

        def tile(r, carry):
            rs = pl.ds(pl.multiple_of(r * RT, RT), RT)
            rows = jnp.concatenate(series_rows(slot, cp, r), axis=1)
            spec = jnp.dot(rows, fwd[table, :], preferred_element_type=F32)
            value = spec.astype(BF16)
            rest = (spec - value.astype(F32)).astype(BF16)
            for q in range(4):
                recv_a[3 - k, q, rs, :] = value[:, q * 128 : (q + 1) * 128]
                recv_a[3 - k, 4 + q, rs, :] = rest[:, q * 128 : (q + 1) * 128]
            return carry

        lax.fori_loop(0, HROWS // RT, tile, 0)
        return carry

    lax.fori_loop(0, 4, partial, 0)

    def late(cp, carry):
        wait_series(0, cp)

        def tile(r, carry):
            rs = pl.ds(pl.multiple_of(r * RT, RT), RT)

            def kept(k):
                return jnp.concatenate(
                    [recv_a[k, q, rs, :].astype(F32) + recv_a[k, 4 + q, rs, :].astype(F32) for q in range(4)],
                    axis=1,
                )

            rows = jnp.concatenate(series_rows(1, cp, r), axis=1)
            spec = jnp.dot(rows, fwd[pl.ds(0, 2 * SC), :], preferred_element_type=F32)
            odd = lax.broadcasted_iota(jnp.int32, (RT, 512), 1) % 2 == 1
            finish(1, cp, r, spec + kept(3 - cp))
            finish(0, cp, r, jnp.where(odd, -spec, spec) + kept(1 - cp))
            return carry

        lax.fori_loop(0, HROWS // RT, tile, 0)
        return carry

    lax.fori_loop(0, 2, late, 0)

    @pl.when(sec == 0)
    def _():
        halo_copy.wait_send()
        halo_b.wait_send()
        to_relay.wait_send()
        for half in range(2):
            sent = send_b.at[CHUNKS - 1, half, :, pl.ds(0, NG // 2)]
            pltpu.make_async_remote_copy(
                sent, sent, sem_mc.at[0, half], sem_mc.at[1, half],
                device_id=(1 - sec, me), device_id_type=MESH,
            ).wait_send()

    @pl.when(sec == 1)
    def _():
        forward.wait_send()

    for t in range(CHUNKS):
        sent = send_a.at[t, pl.ds(0, NG - 1)]
        pltpu.make_async_remote_copy(
            sent, sent, sa_send.at[t], sa_recv.at[t], device_id=(sec, me), device_id_type=MESH
        ).wait_send()
        for cp in range(2):
            sent = send_b.at[t, cp, :, pl.ds(0, NG - 1)]
            pltpu.make_async_remote_copy(
                sent, sent, sb_send.at[t, cp], sb_recv.at[t, cp], device_id=(sec, me), device_id_type=MESH
            ).wait_send()


def local(voltages, filter_taps, beam_weights, antenna_of_row, beam_delay):
    chan_tab = jnp.asarray(channel_tables()).astype(BF16)
    blk_tab = jnp.asarray(block_tables()).astype(BF16)
    ant_row = antenna_of_row.reshape(1, ALL_ANT)
    vmem = pl.BlockSpec(memory_space=pltpu.VMEM)
    smem = pl.BlockSpec(memory_space=pltpu.SMEM)
    hbm = pl.BlockSpec(memory_space=pl.ANY)
    dma = pltpu.SemaphoreType.DMA
    series = pl.pallas_call(
        kernel,
        out_shape=pltpu.VMEM((NG, CPD, 2, BPD, CHUNKS * SC), F32),
        in_specs=[hbm, hbm, hbm, hbm, smem, hbm, hbm],
        out_specs=vmem,
        scratch_shapes=[
            pltpu.VMEM((2, ANT, SC * FRAME + LEAD), BF16),
            pltpu.VMEM((ANT, LEAD), BF16),
            pltpu.VMEM((2, 256, FRAME), BF16),
            pltpu.VMEM((ANT, SC, FRAME), BF16),
            pltpu.VMEM((2, ANT, 256, SC), BF16),
            pltpu.VMEM((CHUNKS, NG, 2 * CPD, ANT, SC), BF16),
            pltpu.VMEM((CHUNKS, 2 * CPD, ALL_ANT, SC), BF16),
            pltpu.VMEM((256, 256), BF16),
            pltpu.VMEM((ALL_ANT, ALL_ANT), BF16),
            pltpu.VMEM((2, BEAMS, ALL_ANT), BF16),
            pltpu.VMEM((2 * CPD, BEAMS, ALL_ANT), BF16),
            pltpu.VMEM((2, 2, BEAMS, SC), F32),
            pltpu.VMEM((CHUNKS, 2, 2, NG, 16, SC), BF16),
            pltpu.VMEM((CHUNKS + 1, 2, 2, NY * NZ, NX, 32, SC), BF16),
            pltpu.VMEM((2, NY * NZ, 32, SC), BF16),
            pltpu.VMEM((2, 2, HROWS, 256), F32),
            pltpu.VMEM((512, 512), BF16),
            pltpu.VMEM((512, 256), BF16),
            pltpu.VMEM((TAPS, FRAME), F32),
            pltpu.VMEM((1, ALL_ANT), jnp.int32),
            pltpu.VMEM((512, HALF), BF16),
            pltpu.VMEM((2, 256, 256), BF16),
            dma((2,)), dma((2,)), dma((4,)), dma((2,)), dma((2,)), dma((2,)), dma((2,)), dma((2, 2)),
            dma((CHUNKS,)), dma((CHUNKS,)), dma((CHUNKS, 2)), dma((CHUNKS, 2)),
        ],
        compiler_params=pltpu.CompilerParams(
            collective_id=0, has_side_effects=True, vmem_limit_bytes=VMEM_LIMIT
        ),
    )(voltages, filter_taps, beam_weights, ant_row, beam_delay, chan_tab, blk_tab)
    return series.reshape(CH, 2, BPD, CHUNKS * SC)


def solution(mesh):
    in_specs = (P("grp", "section"), P(), P("grp", None, None, None), P(), P("grp"))
    out_specs = P(None, None, "grp", "section")
    return jax.shard_map(local, mesh=mesh, in_specs=in_specs, out_specs=out_specs, check_vma=False)
```

```python
import functools
import math
import random

import jax
import jax.numpy as jnp
import numpy as np
from jax import lax
from jax.experimental import pallas as pl
from jax.experimental.pallas import tpu as pltpu
from jax.sharding import PartitionSpec as P

MESH = pl.DeviceIdType.MESH
F32 = jnp.float32
BF16 = jnp.bfloat16
NG = 64
NY, NZ, NX, NC = 4, 4, 2, 2
ANT = 16
FRAME = 512
HALF = FRAME // 2
TAPS = 8
CH = 256
CPD = CH // NG
CHUNKS = 4
SC = 128
LEAD = (TAPS - 1) * FRAME
BEAMS = 512
BPD = BEAMS // NG
ROWS = CH * BPD
ALL_ANT = ANT * NG
HROWS = ROWS // 2
RT = 256
VMEM_LIMIT = 41 * 2**20


def send_order(seed=0):
    rng = random.Random(seed)
    left = [
        (dy, dz, dx, dc) for dy in range(NY) for dz in range(NZ) for dx in range(NX) for dc in range(NC)
    ][1:]
    rng.shuffle(left)
    load = {}

    def ports(o):
        p = []
        for name, d in (("y", o[0]), ("z", o[1])):
            if d in (1, 2):
                p.append(name + "+")
            if d in (2, 3):
                p.append(name + "-")
        if o[2]:
            p.append("x")
        return p

    out = []
    while left:
        best = min(
            left,
            key=lambda o: (max([load.get(p, 0) + 1 for p in ports(o)] + [0]), -len(ports(o)), rng.random()),
        )
        for p in ports(best):
            load[p] = load.get(p, 0) + 1
        out.append(best)
        left.remove(best)
    return out


ORDER = send_order()
CROSS = [o for o in ORDER if o[2]]


def channel_tables():
    j = np.arange(256)
    p = np.arange(HALF)
    tables = []
    for odd in (0, 1):
        channel = (j // 4) * CPD + ((j // 2) % 2) * 2 + odd
        angle = 2.0 * np.pi * ((channel[:, None] * p[None, :]) % FRAME) / FRAME
        value = np.where((j % 2)[:, None] == 0, np.cos(angle), -np.sin(angle)) / math.sqrt(CH)
        tables.append(value.astype(np.float32))
    return np.concatenate(tables, axis=0)


def block_tables():
    n = np.arange(2 * SC)
    angle = 2.0 * np.pi * ((n[:, None] * n[None, :]) % (2 * SC)) / (2 * SC)
    factor = 1.0 / math.sqrt(2 * SC)
    return np.stack([np.cos(angle) * factor, np.sin(angle) * factor]).astype(np.float32)


def disperse_back(spec, chirp, inv, cp, r):
    rs = pl.ds(pl.multiple_of(r * RT, RT), RT)
    sr, si = spec[:, :256], spec[:, 256:]
    cr, ci = chirp[0, cp, rs, :], chirp[1, cp, rs, :]
    filtered = jnp.concatenate([(sr * cr - si * ci).astype(BF16), (sr * ci + si * cr).astype(BF16)], axis=1)
    return jnp.dot(filtered, inv[...], preferred_element_type=F32)


def last_blocks(rows, kept, chirp, fwd, inv, cp, r):
    rs = pl.ds(pl.multiple_of(r * RT, RT), RT)

    def part(k):
        return jnp.concatenate(
            [kept[k, q, rs, :].astype(F32) + kept[k, 4 + q, rs, :].astype(F32) for q in range(4)], axis=1
        )

    spec = jnp.dot(rows, fwd[pl.ds(0, 2 * SC), :], preferred_element_type=F32)
    odd = lax.broadcasted_iota(jnp.int32, (RT, 512), 1) % 2 == 1
    return (
        disperse_back(jnp.where(odd, -spec, spec) + part(1 - cp), chirp, inv, cp, r),
        disperse_back(spec + part(3 - cp), chirp, inv, cp, r),
    )


def finish_kernel(done, kept, chirp, fwd, inv, z_last, out, obuf, sem):
    news = pl.ds(2 * SC, 2 * SC)
    olds = pl.ds(0, 2 * SC)
    copies = [
        pltpu.make_async_copy(done.at[:, :, :, :, news], out.at[:, :, :, :, news], sem.at[0]),
        pltpu.make_async_copy(
            done.at[:, pl.ds(0, 2), :, :, olds], out.at[:, pl.ds(0, 2), :, :, olds], sem.at[1]
        ),
    ]
    for copy in copies:
        copy.start()
    for r in range(HROWS // RT):
        rows = jnp.concatenate([z_last[ri, pl.ds(r * RT, RT), :] for ri in range(2)], axis=1)
        gs = pl.ds(r * (RT // 16), RT // 16)
        for m, res in enumerate(last_blocks(rows, kept, chirp, fwd, inv, 1, r)):
            for ri in range(2):
                part = res[:, ri * SC : (ri + 1) * SC].reshape(RT // 16, 2, BPD, SC)
                for cc in range(2):
                    obuf[gs, cc, ri, :, pl.ds(m * SC, SC)] = part[:, cc]
        copy = pltpu.make_async_copy(
            obuf.at[gs], out.at[gs, pl.ds(2, 2), :, :, olds], sem.at[2 + r]
        )
        copy.start()
        copies.append(copy)
    for copy in copies:
        copy.wait()


def kernel(
    volt, taps_h, weights, ant_row_h, delay, chan_tab_h, blk_tab_h,
    out, recv_a, chirp, fwd, inv, z_last,
    vbuf, halo_a, wblk, wrow, chan, send_a, perm, onehot, wstage, wperm,
    btmp, send_b, recv_b, relay, taps, ant_row, chan_tab, blk_tab,
    sem_v, sem_w, sem_t, sem_ha, sem_hb, sem_rl, sem_fw, sem_mc, sa_send, sa_recv, sb_send, sb_recv,
):
    sec = lax.axis_index("section")
    me = lax.axis_index("grp")
    y, z, x, c = me // (NZ * NX * NC), (me // (NX * NC)) % NZ, (me // NC) % NX, me % NC

    def partner(o):
        dy, dz, dx, dc = o
        return (((y + dy) % NY * NZ + (z + dz) % NZ) * NX + (x + dx) % NX) * NC + (c + dc) % NC

    def load_v(i):
        t = CHUNKS - 1 - i
        return pltpu.make_async_copy(
            volt.at[:, pl.ds(pl.multiple_of(t * (SC * FRAME) - LEAD, 128), SC * FRAME + LEAD)],
            vbuf.at[lax.rem(i, 2)],
            sem_v.at[lax.rem(i, 2)],
        )

    def load_v0():
        return pltpu.make_async_copy(
            volt.at[:, pl.ds(0, SC * FRAME)],
            vbuf.at[(CHUNKS - 1) % 2, :, pl.ds(LEAD, SC * FRAME)],
            sem_v.at[(CHUNKS - 1) % 2],
        )

    def load_w(k):
        return pltpu.make_async_copy(
            weights.at[k // 2, lax.rem(k, 2)], wstage.at[lax.rem(k, 2)], sem_w.at[lax.rem(k, 2)]
        )

    small = [
        pltpu.make_async_copy(src, dst, sem_t.at[n])
        for n, (src, dst) in enumerate(
            ((taps_h, taps), (chan_tab_h, chan_tab), (ant_row_h, ant_row), (blk_tab_h, blk_tab))
        )
    ]

    load_v(0).start()
    for copy in small:
        copy.start()
    load_w(0).start()
    barrier = pltpu.get_barrier_semaphore()
    for o in ORDER:
        pl.semaphore_signal(barrier, inc=1, device_id=(sec, partner(o)), device_id_type=MESH)
    for o in CROSS:
        pl.semaphore_signal(barrier, inc=1, device_id=(1 - sec, partner(o)), device_id_type=MESH)
    pl.semaphore_signal(barrier, inc=1, device_id=(1 - sec, me), device_id_type=MESH)

    row = lax.broadcasted_iota(jnp.int32, (256, 256), 0)
    col = lax.broadcasted_iota(jnp.int32, (256, 256), 1)
    perm[...] = jnp.where((row % 16) * 16 + row // 16 == col, 1.0, 0.0).astype(BF16)
    wblk[...] = jnp.zeros_like(wblk)
    small[0].wait()
    small[1].wait()

    halo_copy = pltpu.make_async_remote_copy(
        volt.at[:, pl.ds(CHUNKS * SC * FRAME - LEAD, LEAD)],
        halo_a,
        sem_ha.at[0],
        sem_ha.at[1],
        device_id=(1 - sec, me),
        device_id_type=MESH,
    )

    def fir_block(slot, sb, wslot):
        base = pl.multiple_of(sb * (16 * FRAME), 16 * FRAME)
        for q in range(2):
            for s0 in (0, 8):
                parts = []
                for p0 in (q * 128, q * 128 + HALF):
                    frames = [
                        vbuf[slot, :, pl.ds(base + (s0 + f) * FRAME + p0, 128)].astype(F32)
                        for f in range(8 + TAPS - 1)
                    ]
                    tap = [taps[pl.ds(k, 1), pl.ds(p0, 128)] for k in range(TAPS)]
                    sums = []
                    for s in range(8):
                        acc = tap[0] * frames[s]
                        for k in range(1, TAPS):
                            acc = acc + tap[k] * frames[s + k]
                        sums.append(acc)
                    parts.append(sums)
                for s in range(8):
                    lo, hi = parts[0][s], parts[1][s]
                    r0 = (s0 + s) * ANT
                    wblk[wslot, pl.ds(r0, ANT), pl.ds(q * 128, 128)] = (lo + hi).astype(BF16)
                    wblk[wslot, pl.ds(r0, ANT), pl.ds(HALF + q * 128, 128)] = (lo - hi).astype(BF16)

    def move_rows(wslot):
        return jnp.dot(perm[...], wblk[wslot], preferred_element_type=F32).reshape(ANT, 16, FRAME).astype(BF16)

    def channelise(i, carry):
        t = CHUNKS - 1 - i
        slot = lax.rem(i, 2)

        @pl.when(i < CHUNKS - 2)
        def _():
            load_v(i + 1).start()

        @pl.when(i == CHUNKS - 2)
        def _():
            load_v0().start()

        @pl.when(i < CHUNKS - 1)
        def _():
            load_v(i).wait()

        @pl.when(i == CHUNKS - 1)
        def _():
            load_v0().wait()

            @pl.when(sec == 1)
            def _():
                halo_copy.wait_recv()

            vbuf[(CHUNKS - 1) % 2, :, pl.ds(0, LEAD)] = halo_a[...]

        def fir(sb, carry):
            moved = move_rows(lax.rem(sb + 1, 2))
            fir_block(slot, sb, lax.rem(sb, 2))
            before = pl.multiple_of(jnp.maximum(sb - 1, 0) * 16, 16)
            wrow[:, pl.ds(before, 16), :] = moved
            return carry

        nblk = SC // 16
        lax.fori_loop(0, nblk, fir, 0)
        wrow[:, pl.ds((nblk - 1) * 16, 16), :] = move_rows((nblk - 1) % 2)

        def dft(ap2, carry):
            for u in range(2):
                ap = ap2 * 2 + u
                rows = wrow[pl.ds(ap * 2, 2)].reshape(2 * SC, FRAME)
                for odd in range(2):
                    res = lax.dot_general(
                        chan_tab[pl.ds(odd * 256, 256), :],
                        rows[:, odd * HALF : (odd + 1) * HALF],
                        (((1,), (1,)), ((), ())),
                        preferred_element_type=F32,
                    ).astype(BF16)
                    chan[odd, ap * 2] = res[:, :SC]
                    chan[odd, ap * 2 + 1] = res[:, SC:]
            return carry

        lax.fori_loop(0, ANT // 4, dft, 0)

        @pl.when(i == 0)
        def _():
            pl.semaphore_wait(barrier, NG + NG // 2)

        mine = pl.ds(pl.multiple_of(me * ANT, ANT), ANT)

        def shift(s):
            return s % NY, (s // NY + s % NY) % NZ

        def regroup(s):
            dy, dz = shift(s)
            jh = (y + dy) % NY * NZ + (z + dz) % NZ
            js = pl.ds(pl.multiple_of(jh * 16, 16), 16)
            both = jnp.concatenate(
                [chan[0, :, js, :].reshape(256, SC), chan[1, :, js, :].reshape(256, SC)], axis=1
            )
            moved = jnp.dot(perm[...], both, preferred_element_type=F32).astype(BF16)
            send_a[t, pl.ds(jh * 4, 4), pl.ds(0, 4)] = moved[:, :SC].reshape(4, 4, ANT, SC)
            send_a[t, pl.ds(jh * 4, 4), pl.ds(4, 4)] = moved[:, SC:].reshape(4, 4, ANT, SC)

        def send(s, r):
            dy, dz = shift(s)
            q = (2 * s + s // NY + r) % (NX * NC)
            to = partner((dy, dz, q // NC, q % NC))
            pltpu.make_async_remote_copy(
                send_a.at[t, to],
                recv_a.at[t, :, mine, :],
                sa_send.at[t],
                sa_recv.at[t],
                device_id=(sec, to),
                device_id_type=MESH,
            ).start()

        nshift = NY * NZ
        regroup(1)

        def step(k, carry):
            regroup(lax.rem(k + 2, nshift))
            send(k + 1, 0)
            return carry

        lax.fori_loop(0, nshift - 1, step, 0)
        pltpu.make_async_copy(send_a.at[t, me], recv_a.at[t, :, mine, :], sa_recv.at[t]).start()

        def rest(r, carry):
            for k in range(nshift):
                send((k + 1) % nshift, r)
            return carry

        lax.fori_loop(1, NX * NC, rest, 0)

        @pl.when((i == 0) & (sec == 0))
        def _():
            halo_copy.start()
            halo_a[...] = jnp.zeros_like(halo_a)
            recv_b[0] = jnp.zeros((2, 2, NY * NZ, NX, 32, SC), BF16)

        return carry

    lax.fori_loop(0, CHUNKS - 1, channelise, 0)

    small[2].wait()

    def build_onehot(k, carry):
        r0 = pl.multiple_of(k * 128, 128)
        antenna = lax.broadcasted_iota(jnp.int32, (128, ALL_ANT), 0) + r0
        onehot[pl.ds(r0, 128), :] = jnp.where(antenna == ant_row[...], 1.0, 0.0).astype(BF16)
        return carry

    lax.fori_loop(0, ALL_ANT // 128, build_onehot, 0)

    def permute_weights(k, carry):
        @pl.when(k < 2 * CPD - 1)
        def _():
            load_w(k + 1).start()

        load_w(k).wait()

        def tile(n, carry):
            cols = pl.ds(pl.multiple_of(n * 256, 256), 256)
            wperm[k, :, cols] = jnp.dot(
                wstage[lax.rem(k, 2)], onehot[:, cols], preferred_element_type=F32
            ).astype(BF16)
            return carry

        lax.fori_loop(0, ALL_ANT // 256, tile, 0)
        return carry

    lax.fori_loop(0, 2 * CPD, permute_weights, 0)

    small[3].wait()
    cos_t, sin_t = blk_tab[0], blk_tab[1]
    for h in range(2):
        part = slice(h * SC, (h + 1) * SC)
        fwd[pl.ds(h * 2 * SC, SC), pl.ds(0, 256)] = cos_t[part, :]
        fwd[pl.ds(h * 2 * SC, SC), pl.ds(256, 256)] = -sin_t[part, :]
        fwd[pl.ds(h * 2 * SC + SC, SC), pl.ds(0, 256)] = sin_t[part, :]
        fwd[pl.ds(h * 2 * SC + SC, SC), pl.ds(256, 256)] = cos_t[part, :]
    inv[pl.ds(0, 256), pl.ds(0, SC)] = cos_t[:, SC:]
    inv[pl.ds(0, 256), pl.ds(SC, SC)] = sin_t[:, SC:]
    inv[pl.ds(256, 256), pl.ds(0, SC)] = -sin_t[:, SC:]
    inv[pl.ds(256, 256), pl.ds(SC, SC)] = cos_t[:, SC:]

    beam = lax.broadcasted_iota(jnp.int32, (BPD, 256), 0)
    dl8 = jnp.zeros((BPD, 256), F32)
    for b in range(BPD):
        dl8 = jnp.where(beam == b, delay[b].astype(F32), dl8)
    dl = jnp.concatenate([dl8] * 8, axis=0)

    def build_chirp(k, carry):
        half, r0 = k // (HROWS // 64), pl.multiple_of(lax.rem(k, HROWS // 64) * 64, 64)
        rows = lax.broadcasted_iota(jnp.int32, (64, 256), 0) + r0
        channel = (rows // 16 * CPD + half * 2 + (rows // BPD) % 2).astype(F32)
        stretch = 1.0 + channel / CH
        strength = 1.0 / (stretch * stretch * stretch)
        f = lax.broadcasted_iota(jnp.int32, (64, 256), 1)
        u = jnp.where(f < SC, f, f - 2 * SC).astype(F32)
        quarters = dl * strength * (u * u) * (1.0 / 32768.0)
        whole = jnp.round(quarters)
        a = (quarters - whole) * (math.pi / 2)
        k4 = (whole.astype(jnp.int32) - f) & 3
        a2 = a * a
        sin_a = a * (1.0 + a2 * (-1.0 / 6 + a2 * (1.0 / 120 + a2 * (-1.0 / 5040 + a2 * (1.0 / 362880)))))
        cos_a = 1.0 + a2 * (
            -0.5 + a2 * (1.0 / 24 + a2 * (-1.0 / 720 + a2 * (1.0 / 40320 + a2 * (-1.0 / 3628800))))
        )
        swap = (k4 & 1) == 1
        cos_p = jnp.where(swap, sin_a, cos_a)
        sin_p = jnp.where(swap, cos_a, sin_a)
        chirp[0, half, pl.ds(r0, 64), :] = jnp.where((k4 == 1) | (k4 == 2), -cos_p, cos_p)
        chirp[1, half, pl.ds(r0, 64), :] = jnp.where(k4 >= 2, -sin_p, sin_p)
        return carry

    lax.fori_loop(0, ROWS // 64, build_chirp, 0)

    own_b = pl.ds(pl.multiple_of(c * 16, 16), 16)
    yz = me // (NX * NC)

    def form(i, carry):
        t = CHUNKS - 1 - i
        got = recv_a.at[t]
        pltpu.make_async_remote_copy(
            got, got, sa_send.at[t], sa_recv.at[t], device_id=(sec, me), device_id_type=MESH
        ).wait_recv()

        def pair(cp, carry):
            for cc in range(2):
                both = jnp.concatenate(
                    [recv_a[t, cc * 4 + cp * 2], recv_a[t, cc * 4 + cp * 2 + 1]], axis=1
                )
                w = cp * 4 + cc * 2
                for h in range(2):
                    bs = pl.ds(h * 256, 256)
                    by_real = jnp.dot(wperm[w, bs, :], both, preferred_element_type=F32)
                    by_imag = jnp.dot(wperm[w + 1, bs, :], both, preferred_element_type=F32)
                    btmp[cc, 0, bs, :] = by_real[:, :SC] - by_imag[:, SC:]
                    btmp[cc, 1, bs, :] = by_real[:, SC:] + by_imag[:, :SC]
            for ri in range(2):
                for h in range(4):
                    joined = jnp.concatenate(
                        [btmp[cc, ri, pl.ds(h * 128, 128), :].reshape(16, BPD, SC) for cc in range(2)],
                        axis=1,
                    )
                    send_b[t, cp, ri, pl.ds(h * 16, 16)] = joined.astype(BF16)
            pltpu.make_async_copy(
                send_b.at[t, cp, :, me], recv_b.at[t + 1, cp, :, yz, x, own_b, :], sb_recv.at[t, cp]
            ).start()
            for o in ORDER:
                to = partner(o)
                pltpu.make_async_remote_copy(
                    send_b.at[t, cp, :, to],
                    recv_b.at[t + 1, cp, :, yz, x, own_b, :],
                    sb_send.at[t, cp],
                    sb_recv.at[t, cp],
                    device_id=(sec, to),
                    device_id_type=MESH,
                ).start()

            @pl.when((i == 0) & (sec == 0))
            def _():
                for o in CROSS:
                    to = partner(o)
                    pltpu.make_async_remote_copy(
                        send_b.at[CHUNKS - 1, cp, :, to],
                        recv_b.at[0, cp, :, yz, x, own_b, :],
                        sem_mc.at[0, cp],
                        sem_mc.at[1, cp],
                        device_id=(1 - sec, to),
                        device_id_type=MESH,
                    ).start()

            return carry

        lax.fori_loop(0, 2, pair, 0)
        return carry

    lax.fori_loop(0, 1, form, 0)
    lax.fori_loop(CHUNKS - 1, CHUNKS, channelise, 0)
    lax.fori_loop(1, CHUNKS - 1, form, 0)

    def wait_series(t, cp):
        got = recv_b.at[t + 1, cp]
        pltpu.make_async_remote_copy(
            got, got, sb_send.at[t, cp], sb_recv.at[t, cp], device_id=(sec, me), device_id_type=MESH
        ).wait_recv()

    flip = partner((0, 0, 1, 0))
    wait_series(CHUNKS - 1, 0)
    wait_series(CHUNKS - 1, 1)
    halo_b = pltpu.make_async_remote_copy(
        recv_b.at[CHUNKS, 0, :, :, x],
        recv_b.at[0, 0, :, :, x],
        sem_hb.at[0],
        sem_hb.at[1],
        device_id=(1 - sec, me),
        device_id_type=MESH,
    )
    to_relay = pltpu.make_async_remote_copy(
        recv_b.at[CHUNKS, 1, :, :, x],
        relay,
        sem_rl.at[0],
        sem_rl.at[1],
        device_id=(1 - sec, flip),
        device_id_type=MESH,
    )
    forward = pltpu.make_async_remote_copy(
        relay,
        recv_b.at[0, 1, :, :, 1 - x],
        sem_fw.at[0],
        sem_fw.at[1],
        device_id=(sec, flip),
        device_id_type=MESH,
    )

    @pl.when(sec == 0)
    def _():
        to_relay.start()
        halo_b.start()

    @pl.when(sec == 1)
    def _():
        to_relay.wait_recv()
        forward.start()

    lax.fori_loop(CHUNKS - 1, CHUNKS, form, 0)

    def series_rows(slot, cp, r):
        qs = pl.ds(r * (RT // 64), RT // 64)
        return [recv_b[slot, cp, ri, qs].reshape(RT, SC) for ri in range(2)]

    def store(m, cp, r, res):
        gs = pl.ds(r * (RT // 16), RT // 16)
        ns = pl.ds(pl.multiple_of(m * SC, SC), SC)
        for ri in range(2):
            part = res[:, ri * SC : (ri + 1) * SC].reshape(RT // 16, 2, BPD, SC)
            for cc in range(2):
                out[gs, cp * 2 + cc, ri, :, ns] = part[:, cc]

    def early(n, carry):
        m, cp = 3 - n // 2, n % 2
        wait_series(m - 1, cp)

        def tile(r, carry):
            block = jnp.concatenate(series_rows(m, cp, r) + series_rows(m + 1, cp, r), axis=1)
            spec = jnp.dot(block, fwd[...], preferred_element_type=F32)
            store(m, cp, r, disperse_back(spec, chirp, inv, cp, r))
            return carry

        lax.fori_loop(0, HROWS // RT, tile, 0)
        return carry

    lax.fori_loop(0, 4, early, 0)

    def partial(k, carry):
        cp, halo = k % 2, k // 2

        @pl.when((k == 2) & (sec == 1))
        def _():
            halo_b.wait_recv()
            pltpu.make_async_remote_copy(
                relay, recv_b.at[0, 1, :, :, x], sem_fw.at[0], sem_fw.at[1],
                device_id=(sec, flip), device_id_type=MESH,
            ).wait_recv()
            for half in range(2):
                got = recv_b.at[0, half, :, :, 1 - x]
                pltpu.make_async_remote_copy(
                    got, got, sem_mc.at[0, half], sem_mc.at[1, half],
                    device_id=(sec, flip), device_id_type=MESH,
                ).wait_recv()

        slot = 2 * (1 - halo)
        table = pl.ds(pl.multiple_of((1 - halo) * 2 * SC, 2 * SC), 2 * SC)

        def tile(r, carry):
            rs = pl.ds(pl.multiple_of(r * RT, RT), RT)
            rows = jnp.concatenate(series_rows(slot, cp, r), axis=1)
            spec = jnp.dot(rows, fwd[table, :], preferred_element_type=F32)
            value = spec.astype(BF16)
            rest = (spec - value.astype(F32)).astype(BF16)
            for q in range(4):
                recv_a[3 - k, q, rs, :] = value[:, q * 128 : (q + 1) * 128]
                recv_a[3 - k, 4 + q, rs, :] = rest[:, q * 128 : (q + 1) * 128]
            return carry

        lax.fori_loop(0, HROWS // RT, tile, 0)
        return carry

    lax.fori_loop(0, 4, partial, 0)

    wait_series(0, 0)

    def late(r, carry):
        rows = jnp.concatenate(series_rows(1, 0, r), axis=1)
        for m, res in enumerate(last_blocks(rows, recv_a, chirp, fwd, inv, 0, r)):
            store(m, 0, r, res)
        return carry

    lax.fori_loop(0, HROWS // RT, late, 0)
    wait_series(0, 1)
    for ri in range(2):
        z_last[ri] = recv_b[1, 1, ri].reshape(HROWS, SC)

    @pl.when(sec == 0)
    def _():
        halo_copy.wait_send()
        halo_b.wait_send()
        to_relay.wait_send()
        for half in range(2):
            sent = send_b.at[CHUNKS - 1, half, :, pl.ds(0, NG // 2)]
            pltpu.make_async_remote_copy(
                sent, sent, sem_mc.at[0, half], sem_mc.at[1, half],
                device_id=(1 - sec, me), device_id_type=MESH,
            ).wait_send()

    @pl.when(sec == 1)
    def _():
        forward.wait_send()

    for t in range(CHUNKS):
        sent = send_a.at[t, pl.ds(0, NG - 1)]
        pltpu.make_async_remote_copy(
            sent, sent, sa_send.at[t], sa_recv.at[t], device_id=(sec, me), device_id_type=MESH
        ).wait_send()
        for cp in range(2):
            sent = send_b.at[t, cp, :, pl.ds(0, NG - 1)]
            pltpu.make_async_remote_copy(
                sent, sent, sb_send.at[t, cp], sb_recv.at[t, cp], device_id=(sec, me), device_id_type=MESH
            ).wait_send()


def local(voltages, filter_taps, beam_weights, antenna_of_row, beam_delay):
    chan_tab = jnp.asarray(channel_tables()).astype(BF16)
    blk_tab = jnp.asarray(block_tables()).astype(BF16)
    ant_row = antenna_of_row.reshape(1, ALL_ANT)
    vmem = pl.BlockSpec(memory_space=pltpu.VMEM)
    smem = pl.BlockSpec(memory_space=pltpu.SMEM)
    hbm = pl.BlockSpec(memory_space=pl.ANY)
    dma = pltpu.SemaphoreType.DMA
    series = pl.pallas_call(
        kernel,
        out_shape=[
            pltpu.VMEM((NG, CPD, 2, BPD, CHUNKS * SC), F32),
            pltpu.VMEM((CHUNKS, 2 * CPD, ALL_ANT, SC), BF16),
            pltpu.VMEM((2, 2, HROWS, 256), F32),
            pltpu.VMEM((512, 512), BF16),
            pltpu.VMEM((512, 256), BF16),
            pltpu.VMEM((2, HROWS, SC), BF16),
        ],
        in_specs=[hbm, hbm, hbm, hbm, smem, hbm, hbm],
        out_specs=[vmem] * 6,
        scratch_shapes=[
            pltpu.VMEM((2, ANT, SC * FRAME + LEAD), BF16),
            pltpu.VMEM((ANT, LEAD), BF16),
            pltpu.VMEM((2, 256, FRAME), BF16),
            pltpu.VMEM((ANT, SC, FRAME), BF16),
            pltpu.VMEM((2, ANT, 256, SC), BF16),
            pltpu.VMEM((CHUNKS, NG, 2 * CPD, ANT, SC), BF16),
            pltpu.VMEM((256, 256), BF16),
            pltpu.VMEM((ALL_ANT, ALL_ANT), BF16),
            pltpu.VMEM((2, BEAMS, ALL_ANT), BF16),
            pltpu.VMEM((2 * CPD, BEAMS, ALL_ANT), BF16),
            pltpu.VMEM((2, 2, BEAMS, SC), F32),
            pltpu.VMEM((CHUNKS, 2, 2, NG, 16, SC), BF16),
            pltpu.VMEM((CHUNKS + 1, 2, 2, NY * NZ, NX, 32, SC), BF16),
            pltpu.VMEM((2, NY * NZ, 32, SC), BF16),
            pltpu.VMEM((TAPS, FRAME), F32),
            pltpu.VMEM((1, ALL_ANT), jnp.int32),
            pltpu.VMEM((512, HALF), BF16),
            pltpu.VMEM((2, 256, 256), BF16),
            dma((2,)), dma((2,)), dma((4,)), dma((2,)), dma((2,)), dma((2,)), dma((2,)), dma((2, 2)),
            dma((CHUNKS,)), dma((CHUNKS,)), dma((CHUNKS, 2)), dma((CHUNKS, 2)),
        ],
        compiler_params=pltpu.CompilerParams(
            collective_id=0, has_side_effects=True, vmem_limit_bytes=VMEM_LIMIT
        ),
    )(voltages, filter_taps, beam_weights, ant_row, beam_delay, chan_tab, blk_tab)
    result = pl.pallas_call(
        finish_kernel,
        out_shape=jax.ShapeDtypeStruct((NG, CPD, 2, BPD, CHUNKS * SC), F32),
        in_specs=[vmem] * 6,
        out_specs=hbm,
        scratch_shapes=[pltpu.VMEM((NG, 2, 2, BPD, 2 * SC), F32), dma((2 + HROWS // RT,))],
        compiler_params=pltpu.CompilerParams(vmem_limit_bytes=8 * 2**20),
    )(*series)
    return result.reshape(CH, 2, BPD, CHUNKS * SC)


def solution(mesh):
    in_specs = (P("grp", "section"), P(), P("grp", None, None, None), P(), P("grp"))
    out_specs = P(None, None, "grp", "section")
    return jax.shard_map(local, mesh=mesh, in_specs=in_specs, out_specs=out_specs, check_vma=False)
```

```python
import functools
import math
import random

import jax
import jax.numpy as jnp
import numpy as np
from jax import lax
from jax.experimental import pallas as pl
from jax.experimental.pallas import tpu as pltpu
from jax.sharding import PartitionSpec as P

MESH = pl.DeviceIdType.MESH
F32 = jnp.float32
BF16 = jnp.bfloat16
NG = 64
NY, NZ, NX, NC = 4, 4, 2, 2
ANT = 16
FRAME = 512
HALF = FRAME // 2
TAPS = 8
CH = 256
CPD = CH // NG
CHUNKS = 4
SC = 128
LEAD = (TAPS - 1) * FRAME
BEAMS = 512
BPD = BEAMS // NG
ROWS = CH * BPD
ALL_ANT = ANT * NG
HROWS = ROWS // 2
RT = 256
VMEM_LIMIT = 41 * 2**20


def send_order(seed=0):
    rng = random.Random(seed)
    left = [
        (dy, dz, dx, dc) for dy in range(NY) for dz in range(NZ) for dx in range(NX) for dc in range(NC)
    ][1:]
    rng.shuffle(left)
    load = {}

    def ports(o):
        p = []
        for name, d in (("y", o[0]), ("z", o[1])):
            if d in (1, 2):
                p.append(name + "+")
            if d in (2, 3):
                p.append(name + "-")
        if o[2]:
            p.append("x")
        return p

    out = []
    while left:
        best = min(
            left,
            key=lambda o: (max([load.get(p, 0) + 1 for p in ports(o)] + [0]), -len(ports(o)), rng.random()),
        )
        for p in ports(best):
            load[p] = load.get(p, 0) + 1
        out.append(best)
        left.remove(best)
    return out


ORDER = send_order()
CROSS = [o for o in ORDER if o[2]]


def channel_tables():
    j = np.arange(256)
    p = np.arange(HALF)
    tables = []
    for odd in (0, 1):
        channel = (j // 4) * CPD + ((j // 2) % 2) * 2 + odd
        angle = 2.0 * np.pi * ((channel[:, None] * p[None, :]) % FRAME) / FRAME
        value = np.where((j % 2)[:, None] == 0, np.cos(angle), -np.sin(angle)) / math.sqrt(CH)
        tables.append(value.astype(np.float32))
    return np.concatenate(tables, axis=0)


def block_tables():
    n = np.arange(2 * SC)
    angle = 2.0 * np.pi * ((n[:, None] * n[None, :]) % (2 * SC)) / (2 * SC)
    factor = 1.0 / math.sqrt(2 * SC)
    return np.stack([np.cos(angle) * factor, np.sin(angle) * factor]).astype(np.float32)


def disperse_back(spec, chirp, inv, cp, r):
    rs = pl.ds(pl.multiple_of(r * RT, RT), RT)
    sr, si = spec[:, :256], spec[:, 256:]
    cr, ci = chirp[0, cp, rs, :], chirp[1, cp, rs, :]
    filtered = jnp.concatenate([(sr * cr - si * ci).astype(BF16), (sr * ci + si * cr).astype(BF16)], axis=1)
    return jnp.dot(filtered, inv[...], preferred_element_type=F32)


def last_blocks(rows, kept, chirp, fwd, inv, cp, r):
    rs = pl.ds(pl.multiple_of(r * RT, RT), RT)

    def part(k):
        return jnp.concatenate(
            [kept[k, q, rs, :].astype(F32) + kept[k, 4 + q, rs, :].astype(F32) for q in range(4)], axis=1
        )

    spec = jnp.dot(rows, fwd[pl.ds(0, 2 * SC), :], preferred_element_type=F32)
    odd = lax.broadcasted_iota(jnp.int32, (RT, 512), 1) % 2 == 1
    return (
        disperse_back(jnp.where(odd, -spec, spec) + part(1 - cp), chirp, inv, cp, r),
        disperse_back(spec + part(3 - cp), chirp, inv, cp, r),
    )


def finish_kernel(done, kept, chirp, fwd, inv, z_last, out, obuf, sem):
    news = pl.ds(2 * SC, 2 * SC)
    olds = pl.ds(0, 2 * SC)
    copies = [
        pltpu.make_async_copy(done.at[:, :, :, :, news], out.at[:, :, :, :, news], sem.at[0]),
        pltpu.make_async_copy(
            done.at[:, pl.ds(0, 2), :, :, olds], out.at[:, pl.ds(0, 2), :, :, olds], sem.at[1]
        ),
    ]
    for copy in copies:
        copy.start()
    for r in range(HROWS // RT):
        rows = jnp.concatenate([z_last[ri, pl.ds(r * RT, RT), :] for ri in range(2)], axis=1)
        gs = pl.ds(r * (RT // 16), RT // 16)
        for m, res in enumerate(last_blocks(rows, kept, chirp, fwd, inv, 1, r)):
            for ri in range(2):
                part = res[:, ri * SC : (ri + 1) * SC].reshape(RT // 16, 2, BPD, SC)
                for cc in range(2):
                    obuf[gs, cc, ri, :, pl.ds(m * SC, SC)] = part[:, cc]
        copy = pltpu.make_async_copy(
            obuf.at[gs], out.at[gs, pl.ds(2, 2), :, :, olds], sem.at[2 + r]
        )
        copy.start()
        copies.append(copy)
    for copy in copies:
        copy.wait()


def kernel(
    volt, taps_h, weights, ant_row_h, delay, chan_tab_h, blk_tab_h,
    out, recv_a, chirp, fwd, inv, z_last,
    vbuf, halo_a, wblk, wrow, chan, send_a, perm, onehot, wstage, wperm,
    btmp, send_b, recv_b, relay, taps, ant_row, chan_tab, blk_tab,
    sem_v, sem_first, sem_w, sem_t, sem_ha, sem_hb, sem_rl, sem_fw, sem_mc, sa_send, sa_recv, sb_send, sb_recv,
):
    sec = lax.axis_index("section")
    me = lax.axis_index("grp")
    y, z, x, c = me // (NZ * NX * NC), (me // (NX * NC)) % NZ, (me // NC) % NX, me % NC

    def partner(o):
        dy, dz, dx, dc = o
        return (((y + dy) % NY * NZ + (z + dz) % NZ) * NX + (x + dx) % NX) * NC + (c + dc) % NC

    def load_v(i):
        t = CHUNKS - 1 - i
        return pltpu.make_async_copy(
            volt.at[:, pl.ds(pl.multiple_of(t * (SC * FRAME) - LEAD, 128), SC * FRAME + LEAD)],
            vbuf.at[lax.rem(i, 2)],
            sem_v.at[lax.rem(i, 2)],
        )

    def load_v0():
        return pltpu.make_async_copy(
            volt.at[:, pl.ds(0, SC * FRAME)],
            vbuf.at[(CHUNKS - 1) % 2, :, pl.ds(LEAD, SC * FRAME)],
            sem_v.at[(CHUNKS - 1) % 2],
        )

    def load_first(n):
        start, size = (0, LEAD + SC * FRAME // 4) if n == 0 else (LEAD + n * (SC * FRAME // 4), SC * FRAME // 4)
        return pltpu.make_async_copy(
            volt.at[:, pl.ds((CHUNKS - 1) * (SC * FRAME) - LEAD + start, size)],
            vbuf.at[0, :, pl.ds(start, size)],
            sem_first.at[n],
        )

    def load_w(k):
        return pltpu.make_async_copy(
            weights.at[k // 2, lax.rem(k, 2)], wstage.at[lax.rem(k, 2)], sem_w.at[lax.rem(k, 2)]
        )

    small = [
        pltpu.make_async_copy(src, dst, sem_t.at[n])
        for n, (src, dst) in enumerate(
            ((taps_h, taps), (chan_tab_h, chan_tab), (ant_row_h, ant_row), (blk_tab_h, blk_tab))
        )
    ]

    load_first(0).start()
    for copy in small:
        copy.start()
    for n in range(1, 4):
        load_first(n).start()
    load_w(0).start()
    barrier = pltpu.get_barrier_semaphore()
    for o in ORDER:
        pl.semaphore_signal(barrier, inc=1, device_id=(sec, partner(o)), device_id_type=MESH)
    for o in CROSS:
        pl.semaphore_signal(barrier, inc=1, device_id=(1 - sec, partner(o)), device_id_type=MESH)
    pl.semaphore_signal(barrier, inc=1, device_id=(1 - sec, me), device_id_type=MESH)

    row = lax.broadcasted_iota(jnp.int32, (256, 256), 0)
    col = lax.broadcasted_iota(jnp.int32, (256, 256), 1)
    perm[...] = jnp.where((row % 16) * 16 + row // 16 == col, 1.0, 0.0).astype(BF16)
    wblk[...] = jnp.zeros_like(wblk)
    small[0].wait()

    halo_copy = pltpu.make_async_remote_copy(
        volt.at[:, pl.ds(CHUNKS * SC * FRAME - LEAD, LEAD)],
        halo_a,
        sem_ha.at[0],
        sem_ha.at[1],
        device_id=(1 - sec, me),
        device_id_type=MESH,
    )

    def fir_block(slot, sb, wslot):
        base = pl.multiple_of(sb * (16 * FRAME), 16 * FRAME)
        for q in range(2):
            for s0 in (0, 8):
                parts = []
                for p0 in (q * 128, q * 128 + HALF):
                    frames = [
                        vbuf[slot, :, pl.ds(base + (s0 + f) * FRAME + p0, 128)].astype(F32)
                        for f in range(8 + TAPS - 1)
                    ]
                    tap = [taps[pl.ds(k, 1), pl.ds(p0, 128)] for k in range(TAPS)]
                    sums = []
                    for s in range(8):
                        acc = tap[0] * frames[s]
                        for k in range(1, TAPS):
                            acc = acc + tap[k] * frames[s + k]
                        sums.append(acc)
                    parts.append(sums)
                for s in range(8):
                    lo, hi = parts[0][s], parts[1][s]
                    r0 = (s0 + s) * ANT
                    wblk[wslot, pl.ds(r0, ANT), pl.ds(q * 128, 128)] = (lo + hi).astype(BF16)
                    wblk[wslot, pl.ds(r0, ANT), pl.ds(HALF + q * 128, 128)] = (lo - hi).astype(BF16)

    def move_rows(wslot):
        return jnp.dot(perm[...], wblk[wslot], preferred_element_type=F32).reshape(ANT, 16, FRAME).astype(BF16)

    def channelise(i, carry):
        t = CHUNKS - 1 - i
        slot = lax.rem(i, 2)

        @pl.when(i < CHUNKS - 2)
        def _():
            load_v(i + 1).start()

        @pl.when(i == CHUNKS - 2)
        def _():
            load_v0().start()

        @pl.when((i > 0) & (i < CHUNKS - 1))
        def _():
            load_v(i).wait()

        @pl.when(i == CHUNKS - 1)
        def _():
            load_v0().wait()

            @pl.when(sec == 1)
            def _():
                halo_copy.wait_recv()

            vbuf[(CHUNKS - 1) % 2, :, pl.ds(0, LEAD)] = halo_a[...]

        def fir(sb, carry):
            for n in range(4):

                @pl.when((i == 0) & (sb == 2 * n))
                def _():
                    load_first(n).wait()

            moved = move_rows(lax.rem(sb + 1, 2))
            fir_block(slot, sb, lax.rem(sb, 2))
            before = pl.multiple_of(jnp.maximum(sb - 1, 0) * 16, 16)
            wrow[:, pl.ds(before, 16), :] = moved
            return carry

        nblk = SC // 16
        lax.fori_loop(0, nblk, fir, 0)
        wrow[:, pl.ds((nblk - 1) * 16, 16), :] = move_rows((nblk - 1) % 2)

        @pl.when(i == 0)
        def _():
            small[1].wait()

        def dft(ap2, carry):
            for u in range(2):
                ap = ap2 * 2 + u
                rows = wrow[pl.ds(ap * 2, 2)].reshape(2 * SC, FRAME)
                for odd in range(2):
                    res = lax.dot_general(
                        chan_tab[pl.ds(odd * 256, 256), :],
                        rows[:, odd * HALF : (odd + 1) * HALF],
                        (((1,), (1,)), ((), ())),
                        preferred_element_type=F32,
                    ).astype(BF16)
                    chan[odd, ap * 2] = res[:, :SC]
                    chan[odd, ap * 2 + 1] = res[:, SC:]
            return carry

        lax.fori_loop(0, ANT // 4, dft, 0)

        @pl.when(i == 0)
        def _():
            pl.semaphore_wait(barrier, NG + NG // 2)

        mine = pl.ds(pl.multiple_of(me * ANT, ANT), ANT)

        def shift(s):
            return s % NY, (s // NY + s % NY) % NZ

        def regroup(s):
            dy, dz = shift(s)
            jh = (y + dy) % NY * NZ + (z + dz) % NZ
            js = pl.ds(pl.multiple_of(jh * 16, 16), 16)
            both = jnp.concatenate(
                [chan[0, :, js, :].reshape(256, SC), chan[1, :, js, :].reshape(256, SC)], axis=1
            )
            moved = jnp.dot(perm[...], both, preferred_element_type=F32).astype(BF16)
            send_a[t, pl.ds(jh * 4, 4), pl.ds(0, 4)] = moved[:, :SC].reshape(4, 4, ANT, SC)
            send_a[t, pl.ds(jh * 4, 4), pl.ds(4, 4)] = moved[:, SC:].reshape(4, 4, ANT, SC)

        def send(s, r):
            dy, dz = shift(s)
            q = (2 * s + s // NY + r) % (NX * NC)
            to = partner((dy, dz, q // NC, q % NC))
            pltpu.make_async_remote_copy(
                send_a.at[t, to],
                recv_a.at[t, :, mine, :],
                sa_send.at[t],
                sa_recv.at[t],
                device_id=(sec, to),
                device_id_type=MESH,
            ).start()

        nshift = NY * NZ
        regroup(1)

        def step(k, carry):
            regroup(lax.rem(k + 2, nshift))
            send(k + 1, 0)
            return carry

        lax.fori_loop(0, nshift - 1, step, 0)
        pltpu.make_async_copy(send_a.at[t, me], recv_a.at[t, :, mine, :], sa_recv.at[t]).start()

        def rest(r, carry):
            for k in range(nshift):
                send((k + 1) % nshift, r)
            return carry

        lax.fori_loop(1, NX * NC, rest, 0)

        @pl.when((i == 0) & (sec == 0))
        def _():
            halo_copy.start()
            halo_a[...] = jnp.zeros_like(halo_a)
            recv_b[0] = jnp.zeros((2, 2, NY * NZ, NX, 32, SC), BF16)

        return carry

    lax.fori_loop(0, CHUNKS - 1, channelise, 0)

    small[2].wait()

    def build_onehot(k, carry):
        r0 = pl.multiple_of(k * 128, 128)
        antenna = lax.broadcasted_iota(jnp.int32, (128, ALL_ANT), 0) + r0
        onehot[pl.ds(r0, 128), :] = jnp.where(antenna == ant_row[...], 1.0, 0.0).astype(BF16)
        return carry

    lax.fori_loop(0, ALL_ANT // 128, build_onehot, 0)

    def permute_weights(k, carry):
        @pl.when(k < 2 * CPD - 1)
        def _():
            load_w(k + 1).start()

        load_w(k).wait()

        def tile(n, carry):
            cols = pl.ds(pl.multiple_of(n * 256, 256), 256)
            wperm[k, :, cols] = jnp.dot(
                wstage[lax.rem(k, 2)], onehot[:, cols], preferred_element_type=F32
            ).astype(BF16)
            return carry

        lax.fori_loop(0, ALL_ANT // 256, tile, 0)
        return carry

    lax.fori_loop(0, 2 * CPD, permute_weights, 0)

    small[3].wait()
    cos_t, sin_t = blk_tab[0], blk_tab[1]
    for h in range(2):
        part = slice(h * SC, (h + 1) * SC)
        fwd[pl.ds(h * 2 * SC, SC), pl.ds(0, 256)] = cos_t[part, :]
        fwd[pl.ds(h * 2 * SC, SC), pl.ds(256, 256)] = -sin_t[part, :]
        fwd[pl.ds(h * 2 * SC + SC, SC), pl.ds(0, 256)] = sin_t[part, :]
        fwd[pl.ds(h * 2 * SC + SC, SC), pl.ds(256, 256)] = cos_t[part, :]
    inv[pl.ds(0, 256), pl.ds(0, SC)] = cos_t[:, SC:]
    inv[pl.ds(0, 256), pl.ds(SC, SC)] = sin_t[:, SC:]
    inv[pl.ds(256, 256), pl.ds(0, SC)] = -sin_t[:, SC:]
    inv[pl.ds(256, 256), pl.ds(SC, SC)] = cos_t[:, SC:]

    beam = lax.broadcasted_iota(jnp.int32, (BPD, 256), 0)
    dl8 = jnp.zeros((BPD, 256), F32)
    for b in range(BPD):
        dl8 = jnp.where(beam == b, delay[b].astype(F32), dl8)
    dl = jnp.concatenate([dl8] * 8, axis=0)

    def build_chirp(k, carry):
        half, r0 = k // (HROWS // 64), pl.multiple_of(lax.rem(k, HROWS // 64) * 64, 64)
        rows = lax.broadcasted_iota(jnp.int32, (64, 256), 0) + r0
        channel = (rows // 16 * CPD + half * 2 + (rows // BPD) % 2).astype(F32)
        stretch = 1.0 + channel / CH
        strength = 1.0 / (stretch * stretch * stretch)
        f = lax.broadcasted_iota(jnp.int32, (64, 256), 1)
        u = jnp.where(f < SC, f, f - 2 * SC).astype(F32)
        quarters = dl * strength * (u * u) * (1.0 / 32768.0)
        whole = jnp.round(quarters)
        a = (quarters - whole) * (math.pi / 2)
        k4 = (whole.astype(jnp.int32) - f) & 3
        a2 = a * a
        sin_a = a * (1.0 + a2 * (-1.0 / 6 + a2 * (1.0 / 120 + a2 * (-1.0 / 5040 + a2 * (1.0 / 362880)))))
        cos_a = 1.0 + a2 * (
            -0.5 + a2 * (1.0 / 24 + a2 * (-1.0 / 720 + a2 * (1.0 / 40320 + a2 * (-1.0 / 3628800))))
        )
        swap = (k4 & 1) == 1
        cos_p = jnp.where(swap, sin_a, cos_a)
        sin_p = jnp.where(swap, cos_a, sin_a)
        chirp[0, half, pl.ds(r0, 64), :] = jnp.where((k4 == 1) | (k4 == 2), -cos_p, cos_p)
        chirp[1, half, pl.ds(r0, 64), :] = jnp.where(k4 >= 2, -sin_p, sin_p)
        return carry

    lax.fori_loop(0, ROWS // 64, build_chirp, 0)

    own_b = pl.ds(pl.multiple_of(c * 16, 16), 16)
    yz = me // (NX * NC)

    def form(i, carry):
        t = CHUNKS - 1 - i
        got = recv_a.at[t]
        pltpu.make_async_remote_copy(
            got, got, sa_send.at[t], sa_recv.at[t], device_id=(sec, me), device_id_type=MESH
        ).wait_recv()

        def pair(cp, carry):
            for cc in range(2):
                both = jnp.concatenate(
                    [recv_a[t, cc * 4 + cp * 2], recv_a[t, cc * 4 + cp * 2 + 1]], axis=1
                )
                w = cp * 4 + cc * 2
                for h in range(2):
                    bs = pl.ds(h * 256, 256)
                    by_real = jnp.dot(wperm[w, bs, :], both, preferred_element_type=F32)
                    by_imag = jnp.dot(wperm[w + 1, bs, :], both, preferred_element_type=F32)
                    btmp[cc, 0, bs, :] = by_real[:, :SC] - by_imag[:, SC:]
                    btmp[cc, 1, bs, :] = by_real[:, SC:] + by_imag[:, :SC]
            for ri in range(2):
                for h in range(4):
                    joined = jnp.concatenate(
                        [btmp[cc, ri, pl.ds(h * 128, 128), :].reshape(16, BPD, SC) for cc in range(2)],
                        axis=1,
                    )
                    send_b[t, cp, ri, pl.ds(h * 16, 16)] = joined.astype(BF16)
            pltpu.make_async_copy(
                send_b.at[t, cp, :, me], recv_b.at[t + 1, cp, :, yz, x, own_b, :], sb_recv.at[t, cp]
            ).start()
            for o in ORDER:
                to = partner(o)
                pltpu.make_async_remote_copy(
                    send_b.at[t, cp, :, to],
                    recv_b.at[t + 1, cp, :, yz, x, own_b, :],
                    sb_send.at[t, cp],
                    sb_recv.at[t, cp],
                    device_id=(sec, to),
                    device_id_type=MESH,
                ).start()

            @pl.when((i == 0) & (sec == 0))
            def _():
                for o in CROSS:
                    to = partner(o)
                    pltpu.make_async_remote_copy(
                        send_b.at[CHUNKS - 1, cp, :, to],
                        recv_b.at[0, cp, :, yz, x, own_b, :],
                        sem_mc.at[0, cp],
                        sem_mc.at[1, cp],
                        device_id=(1 - sec, to),
                        device_id_type=MESH,
                    ).start()

            return carry

        lax.fori_loop(0, 2, pair, 0)
        return carry

    lax.fori_loop(0, 1, form, 0)
    lax.fori_loop(CHUNKS - 1, CHUNKS, channelise, 0)
    lax.fori_loop(1, CHUNKS - 1, form, 0)

    def wait_series(t, cp):
        got = recv_b.at[t + 1, cp]
        pltpu.make_async_remote_copy(
            got, got, sb_send.at[t, cp], sb_recv.at[t, cp], device_id=(sec, me), device_id_type=MESH
        ).wait_recv()

    flip = partner((0, 0, 1, 0))
    wait_series(CHUNKS - 1, 0)
    wait_series(CHUNKS - 1, 1)
    halo_b = pltpu.make_async_remote_copy(
        recv_b.at[CHUNKS, 0, :, :, x],
        recv_b.at[0, 0, :, :, x],
        sem_hb.at[0],
        sem_hb.at[1],
        device_id=(1 - sec, me),
        device_id_type=MESH,
    )
    to_relay = pltpu.make_async_remote_copy(
        recv_b.at[CHUNKS, 1, :, :, x],
        relay,
        sem_rl.at[0],
        sem_rl.at[1],
        device_id=(1 - sec, flip),
        device_id_type=MESH,
    )
    forward = pltpu.make_async_remote_copy(
        relay,
        recv_b.at[0, 1, :, :, 1 - x],
        sem_fw.at[0],
        sem_fw.at[1],
        device_id=(sec, flip),
        device_id_type=MESH,
    )

    @pl.when(sec == 0)
    def _():
        to_relay.start()
        halo_b.start()

    @pl.when(sec == 1)
    def _():
        to_relay.wait_recv()
        forward.start()

    lax.fori_loop(CHUNKS - 1, CHUNKS, form, 0)

    def series_rows(slot, cp, r):
        qs = pl.ds(r * (RT // 64), RT // 64)
        return [recv_b[slot, cp, ri, qs].reshape(RT, SC) for ri in range(2)]

    def store(m, cp, r, res):
        gs = pl.ds(r * (RT // 16), RT // 16)
        ns = pl.ds(pl.multiple_of(m * SC, SC), SC)
        for ri in range(2):
            part = res[:, ri * SC : (ri + 1) * SC].reshape(RT // 16, 2, BPD, SC)
            for cc in range(2):
                out[gs, cp * 2 + cc, ri, :, ns] = part[:, cc]

    def early(n, carry):
        m, cp = 3 - n // 2, n % 2
        wait_series(m - 1, cp)

        def tile(r, carry):
            block = jnp.concatenate(series_rows(m, cp, r) + series_rows(m + 1, cp, r), axis=1)
            spec = jnp.dot(block, fwd[...], preferred_element_type=F32)
            store(m, cp, r, disperse_back(spec, chirp, inv, cp, r))
            return carry

        lax.fori_loop(0, HROWS // RT, tile, 0)
        return carry

    lax.fori_loop(0, 4, early, 0)

    def partial(k, carry):
        cp, halo = k % 2, k // 2

        @pl.when((k == 2) & (sec == 1))
        def _():
            halo_b.wait_recv()
            pltpu.make_async_remote_copy(
                relay, recv_b.at[0, 1, :, :, x], sem_fw.at[0], sem_fw.at[1],
                device_id=(sec, flip), device_id_type=MESH,
            ).wait_recv()
            for half in range(2):
                got = recv_b.at[0, half, :, :, 1 - x]
                pltpu.make_async_remote_copy(
                    got, got, sem_mc.at[0, half], sem_mc.at[1, half],
                    device_id=(sec, flip), device_id_type=MESH,
                ).wait_recv()

        slot = 2 * (1 - halo)
        table = pl.ds(pl.multiple_of((1 - halo) * 2 * SC, 2 * SC), 2 * SC)

        def tile(r, carry):
            rs = pl.ds(pl.multiple_of(r * RT, RT), RT)
            rows = jnp.concatenate(series_rows(slot, cp, r), axis=1)
            spec = jnp.dot(rows, fwd[table, :], preferred_element_type=F32)
            value = spec.astype(BF16)
            rest = (spec - value.astype(F32)).astype(BF16)
            for q in range(4):
                recv_a[3 - k, q, rs, :] = value[:, q * 128 : (q + 1) * 128]
                recv_a[3 - k, 4 + q, rs, :] = rest[:, q * 128 : (q + 1) * 128]
            return carry

        lax.fori_loop(0, HROWS // RT, tile, 0)
        return carry

    lax.fori_loop(0, 4, partial, 0)

    wait_series(0, 0)

    def late(r, carry):
        rows = jnp.concatenate(series_rows(1, 0, r), axis=1)
        for m, res in enumerate(last_blocks(rows, recv_a, chirp, fwd, inv, 0, r)):
            store(m, 0, r, res)
        return carry

    lax.fori_loop(0, HROWS // RT, late, 0)
    wait_series(0, 1)
    for ri in range(2):
        z_last[ri] = recv_b[1, 1, ri].reshape(HROWS, SC)

    @pl.when(sec == 0)
    def _():
        halo_copy.wait_send()
        halo_b.wait_send()
        to_relay.wait_send()
        for half in range(2):
            sent = send_b.at[CHUNKS - 1, half, :, pl.ds(0, NG // 2)]
            pltpu.make_async_remote_copy(
                sent, sent, sem_mc.at[0, half], sem_mc.at[1, half],
                device_id=(1 - sec, me), device_id_type=MESH,
            ).wait_send()

    @pl.when(sec == 1)
    def _():
        forward.wait_send()

    for t in range(CHUNKS):
        sent = send_a.at[t, pl.ds(0, NG - 1)]
        pltpu.make_async_remote_copy(
            sent, sent, sa_send.at[t], sa_recv.at[t], device_id=(sec, me), device_id_type=MESH
        ).wait_send()
        for cp in range(2):
            sent = send_b.at[t, cp, :, pl.ds(0, NG - 1)]
            pltpu.make_async_remote_copy(
                sent, sent, sb_send.at[t, cp], sb_recv.at[t, cp], device_id=(sec, me), device_id_type=MESH
            ).wait_send()


def local(voltages, filter_taps, beam_weights, antenna_of_row, beam_delay):
    chan_tab = jnp.asarray(channel_tables()).astype(BF16)
    blk_tab = jnp.asarray(block_tables()).astype(BF16)
    ant_row = antenna_of_row.reshape(1, ALL_ANT)
    vmem = pl.BlockSpec(memory_space=pltpu.VMEM)
    smem = pl.BlockSpec(memory_space=pltpu.SMEM)
    hbm = pl.BlockSpec(memory_space=pl.ANY)
    dma = pltpu.SemaphoreType.DMA
    series = pl.pallas_call(
        kernel,
        out_shape=[
            pltpu.VMEM((NG, CPD, 2, BPD, CHUNKS * SC), F32),
            pltpu.VMEM((CHUNKS, 2 * CPD, ALL_ANT, SC), BF16),
            pltpu.VMEM((2, 2, HROWS, 256), F32),
            pltpu.VMEM((512, 512), BF16),
            pltpu.VMEM((512, 256), BF16),
            pltpu.VMEM((2, HROWS, SC), BF16),
        ],
        in_specs=[hbm, hbm, hbm, hbm, smem, hbm, hbm],
        out_specs=[vmem] * 6,
        scratch_shapes=[
            pltpu.VMEM((2, ANT, SC * FRAME + LEAD), BF16),
            pltpu.VMEM((ANT, LEAD), BF16),
            pltpu.VMEM((2, 256, FRAME), BF16),
            pltpu.VMEM((ANT, SC, FRAME), BF16),
            pltpu.VMEM((2, ANT, 256, SC), BF16),
            pltpu.VMEM((CHUNKS, NG, 2 * CPD, ANT, SC), BF16),
            pltpu.VMEM((256, 256), BF16),
            pltpu.VMEM((ALL_ANT, ALL_ANT), BF16),
            pltpu.VMEM((2, BEAMS, ALL_ANT), BF16),
            pltpu.VMEM((2 * CPD, BEAMS, ALL_ANT), BF16),
            pltpu.VMEM((2, 2, BEAMS, SC), F32),
            pltpu.VMEM((CHUNKS, 2, 2, NG, 16, SC), BF16),
            pltpu.VMEM((CHUNKS + 1, 2, 2, NY * NZ, NX, 32, SC), BF16),
            pltpu.VMEM((2, NY * NZ, 32, SC), BF16),
            pltpu.VMEM((TAPS, FRAME), F32),
            pltpu.VMEM((1, ALL_ANT), jnp.int32),
            pltpu.VMEM((512, HALF), BF16),
            pltpu.VMEM((2, 256, 256), BF16),
            dma((2,)), dma((4,)), dma((2,)), dma((4,)), dma((2,)), dma((2,)), dma((2,)), dma((2,)), dma((2, 2)),
            dma((CHUNKS,)), dma((CHUNKS,)), dma((CHUNKS, 2)), dma((CHUNKS, 2)),
        ],
        compiler_params=pltpu.CompilerParams(
            collective_id=0, has_side_effects=True, vmem_limit_bytes=VMEM_LIMIT
        ),
    )(voltages, filter_taps, beam_weights, ant_row, beam_delay, chan_tab, blk_tab)
    result = pl.pallas_call(
        finish_kernel,
        out_shape=jax.ShapeDtypeStruct((NG, CPD, 2, BPD, CHUNKS * SC), F32),
        in_specs=[vmem] * 6,
        out_specs=hbm,
        scratch_shapes=[pltpu.VMEM((NG, 2, 2, BPD, 2 * SC), F32), dma((2 + HROWS // RT,))],
        compiler_params=pltpu.CompilerParams(vmem_limit_bytes=8 * 2**20),
    )(*series)
    return result.reshape(CH, 2, BPD, CHUNKS * SC)


def solution(mesh):
    in_specs = (P("grp", "section"), P(), P("grp", None, None, None), P(), P("grp"))
    out_specs = P(None, None, "grp", "section")
    return jax.shard_map(local, mesh=mesh, in_specs=in_specs, out_specs=out_specs, check_vma=False)
```
